256 devices in a mesh: bank: 32 (over z_hi, y, x), lane: 8 (over z_lo, core).
Axes of the slice: x: 4, y: 4, z: 8 (z_hi: 2, z_lo: 4; z = z_hi * 4 + z_lo), core: 2. Of those that a mesh axis runs over, the one named last changes fastest.
Arguments:
- amplitudes: float32 [2, 1024, 128, 128], P(None, ('bank', 'lane')), may hold values from -6 to 6
- energies: float32 [1024, 128, 128], P(('bank', 'lane')), may hold values from -2 to 2
- phase_angles: float32 [2, 128], replicated, may hold values from 0.3 to 1.2
- mix_angles: float32 [2, 4], replicated, may hold values from 0.3 to 1.2
Outputs:
- final_parts: float32 [2, 1024, 128, 128], P(None, ('bank', 'lane'))
- marginal: float32 [32, 128, 128], P('lane', 'bank')
The draws below stay inside these ranges and needn't reach their ends.
All inputs are finite; a program needn't handle non-finite values.
Results may differ from the reference program's by a relative error of at most 0.0003.
Values sent between devices are 32-bit elements; how exact they have to be, the bound alone decides.
No kernel may reach another device: no remote copies, remote signals or barrier semaphores. Data moves between devices by JAX's collectives and lax.ppermute only.
A program may use at most 64 MiB of HBM per device.

```python
import jax
import jax.numpy as jnp
from jax import lax

BLOCKS_DEV = 4
ROWS = 128
LANES = 128
BLOCKS = 1024
LAYERS = 2
N_BANK = 32
N_LANE = 8


def steps_of(stream_key, dims, pieces, low, top_value):
    def one(axis_at, shards_of):
        heights = jax.random.uniform(jax.random.fold_in(jax.random.fold_in(stream_key, 6), axis_at), (shards_of,), jnp.float32, low / len(pieces), top_value / len(pieces))
        return jnp.repeat(jnp.exp(heights), dims[axis_at] // shards_of).reshape((-1,) + (1,) * (len(dims) - axis_at - 1))

    loudness = one(*pieces[0])
    for cut in pieces[1:]:
        loudness = loudness * one(*cut)
    return loudness


def noise(key, dims, spread, bound, shards=(), kind=jnp.bfloat16):
    entries = jax.random.normal(key, dims, jnp.float32) * spread
    if len(shards) > 0:
        entries = steps_of(key, dims, shards, -0.22, 0.18) * entries
    return jnp.clip(entries, min=-bound, max=bound).astype(kind)


def setup_inputs(seed: int = 0) -> dict:
    key_list = jax.random.split(jax.random.key(seed), 5)
    return {
        "amplitudes": noise(key_list[0], (2, BLOCKS, ROWS, LANES), 1.0, 6.0, ((1, 256),), jnp.float32),
        "energies": jnp.clip(jax.random.uniform(key_list[1], (BLOCKS, ROWS, LANES), jnp.float32, -2.0, 2.0) * steps_of(key_list[1], (BLOCKS, ROWS, LANES), ((0, 256),), -0.4, 0.0), -2.0, 2.0),
        "phase_angles": jnp.clip(jax.random.uniform(key_list[2], (LAYERS, LANES), jnp.float32, 0.3, 1.2), 0.3, 1.2),
        "mix_angles": jnp.clip(jax.random.uniform(key_list[3], (LAYERS, 4), jnp.float32, 0.3, 1.2), 0.3, 1.2),
    }


def count_bits(values, count):
    places = jnp.arange(count.bit_length() - 1, dtype=jnp.int32)
    return jnp.sum((values[..., None] >> places) & 1, axis=-1)


def turn_table(count, angle):
    rank = jnp.arange(count, dtype=jnp.int32)
    apart = count_bits(rank[:, None] ^ rank[None, :], count)
    bits = count.bit_length() - 1
    size = jnp.cos(angle) ** (bits - apart).astype(jnp.float32) * jnp.sin(angle) ** apart.astype(jnp.float32)
    real_sign = jnp.where(apart % 4 == 0, 1.0, jnp.where(apart % 4 == 2, -1.0, 0.0)).astype(jnp.float32)
    imag_sign = jnp.where(apart % 4 == 1, -1.0, jnp.where(apart % 4 == 3, 1.0, 0.0)).astype(jnp.float32)
    return size * real_sign, size * imag_sign


def apply_along(values, dim, angle):
    real_part, imag_part = turn_table(values.shape[dim], angle)
    def times(table):
        moved = jnp.tensordot(values, table, axes=([dim], [0]), precision=lax.Precision.HIGHEST)
        return jnp.moveaxis(moved, -1, dim)
    by_real = times(real_part)
    by_imag = times(imag_part)
    return jnp.stack([by_real[0] - by_imag[1], by_real[1] + by_imag[0]])


def diagonal_step(values, levels, angle):
    turn = angle * levels
    return jnp.stack([values[0] * jnp.cos(turn) + values[1] * jnp.sin(turn), values[1] * jnp.cos(turn) - values[0] * jnp.sin(turn)])


def reference(amplitudes, energies, phase_angles, mix_angles):
    values = amplitudes
    for layer in range(LAYERS):
        values = diagonal_step(values, energies, phase_angles[layer])
        values = apply_along(values, 3, mix_angles[layer, 0])
        values = apply_along(values, 2, mix_angles[layer, 1])
        parts = values.reshape(2, N_BANK, N_LANE, BLOCKS_DEV, ROWS, LANES)
        parts = apply_along(parts, 1, mix_angles[layer, 2])
        parts = apply_along(parts, 2, mix_angles[layer, 3])
        parts = apply_along(parts, 3, mix_angles[layer, 2])
        values = parts.reshape(values.shape)
    chance = values[0] * values[0] + values[1] * values[1]
    marginal = jnp.mean(chance.reshape(N_BANK, -1, ROWS, LANES), axis=0)
    return values, marginal
```

```python
import jax
import jax.numpy as jnp
from jax import lax
from jax.experimental import pallas as pl
from jax.experimental.pallas import tpu as pltpu
from jax.sharding import PartitionSpec as P


ROT, ROT_T, FLIP = 0, 1, 2
GROUP = ("lane", "bank")


def trig(x):
    y = x * x
    c = jnp.full_like(x, 1.0 / 20922789888000.0)
    s = jnp.full_like(x, 1.0 / 355687428096000.0)
    for k in (-87178291200.0, 479001600.0, -3628800.0, 40320.0, -720.0, 24.0, -2.0, 1.0):
        c = c * y + 1.0 / k
    for k in (-1307674368000.0, 6227020800.0, -39916800.0, 362880.0, -5040.0, 120.0, -6.0, 1.0):
        s = s * y + 1.0 / k
    return c, s * x


def angle(mix_ref, layer, group, width=128):
    return trig(jnp.full((1, width), mix_ref[layer, group], jnp.float32))


def iota(shape, dim):
    return lax.broadcasted_iota(jnp.int32, shape, dim)


def bit(value, k):
    return (value >> k) & 1


def pop(value, bits):
    total = bit(value, 0)
    for k in range(1, bits):
        total = total + bit(value, k)
    return total


def pair(kind, c, s):
    if kind == ROT:
        return c, s, -s, c
    if kind == ROT_T:
        return c, -s, s, c
    return c, s, s, -c


def table(shape, pairs):
    i, j = iota(shape, 0), iota(shape, 1)
    out = None
    for ki, kj, kind, c, s in pairs:
        a00, a01, a10, a11 = pair(kind, c, s)
        odd = bit(j, kj) == 1
        part = jnp.where(bit(i, ki) == 1, jnp.where(odd, a11, a10), jnp.where(odd, a01, a00))
        out = part if out is None else out * part
    return out


def doubled(small, kind, c, s):
    a00, a01, a10, a11 = pair(kind, c, s)
    top = jnp.concatenate([small * a00, small * a01], axis=1)
    low = jnp.concatenate([small * a10, small * a11], axis=1)
    return jnp.concatenate([top, low], axis=0)


def halves(x):
    high = x.astype(jnp.bfloat16)
    return high, (x - high.astype(jnp.float32)).astype(jnp.bfloat16)


def mm(a, b):
    ah, al = halves(a)
    bh, bl = halves(b)

    def one(p, q):
        return jnp.dot(p, q, preferred_element_type=jnp.float32)

    return one(ah, bh) + (one(ah, bl) + one(al, bh))


def own_pop():
    return pop(lax.axis_index("bank"), 5) + pop(lax.axis_index("lane"), 3)


def quarter_turns(extra):
    shape = (128, 128)
    p = pop(iota(shape, 0), 7) + pop(iota(shape, 1), 7) + extra
    return bit(p, 0) == 1, 1.0 - 2.0 * bit(p, 1).astype(jnp.float32)


def first_kernel(amp, en, ph, mix, out):
    own = own_pop()
    turns = [quarter_turns(own + k) for k in range(3)]
    xr, xi = [], []
    for t in range(4):
        odd, sign = turns[bin(t).count("1")]
        e = en[t]
        c, s = trig(ph[0:1, :] * e)
        c, s = jnp.where(odd, -s, c) * sign, jnp.where(odd, c, s) * sign
        re, im = amp[0, t], amp[1, t]
        xr.append(re * c + im * s)
        xi.append(im * c - re * s)
        e2 = (ph[1:2, :] * e).T
        for lb in range(2):
            out[pl.ds(t * 64 * 6 + 4 + lb, 64, stride=6), :] = e2[lb * 64 : lb * 64 + 64]
    c, s = angle(mix, 0, 2)
    x = []
    for v in (xr, xi):
        v = [c * v[0] + s * v[1], c * v[1] - s * v[0], c * v[2] + s * v[3], c * v[3] - s * v[2]]
        x += [c * v[0] + s * v[2], c * v[1] + s * v[3], c * v[2] - s * v[0], c * v[3] - s * v[1]]
    c, s = angle(mix, 0, 0)
    lanes = table((128, 128), [(k, k, ROT_T, c, s) for k in range(7)])
    c, s = angle(mix, 0, 1)
    rows = table((128, 128), [(k, k, ROT_T, c, s) for k in range(7)])
    y = mm(jnp.concatenate(x, axis=0), lanes)
    y = jnp.concatenate([y[k * 128 : k * 128 + 128].T for k in range(8)], axis=0)
    y = mm(y, rows)
    for c in range(2):
        for t in range(4):
            for lb in range(2):
                at = (c * 4 + t) * 128 + lb * 64
                out[pl.ds(t * 64 * 6 + c * 2 + lb, 64, stride=6), :] = y[at : at + 64]


def device_bits(mix, layer, kind):
    c2, s2 = angle(mix, layer, 2)
    c3, s3 = angle(mix, layer, 3)
    small = table(
        (128, 128), [(k, k, kind, c2, s2) for k in range(5)] + [(k, k, kind, c3, s3) for k in (5, 6)]
    )
    return doubled(small, kind, c3, s3)


def second_kernel(arrived, mix, out):
    x = jnp.concatenate([arrived[pl.ds(k, 256, stride=6), :] for k in range(4)], axis=1)
    y = mm(device_bits(mix, 0, ROT), x)
    z = [None] * 4
    for lb in range(2):
        c, s = trig(arrived[pl.ds(4 + lb, 256, stride=6), :])
        re, im = y[:, lb * 128 : lb * 128 + 128], y[:, 256 + lb * 128 : 384 + lb * 128]
        z[lb] = re * c + im * s
        z[2 + lb] = im * c - re * s
    c1, s1 = angle(mix, 1, 1)
    moved = (5, 6, 0, 1, 2, 3, 4)
    rows = table((128, 128), [(k, moved[k], FLIP, c1, s1) for k in range(7)])
    c0, s0 = angle(mix, 1, 0)
    z = jnp.concatenate(
        [jnp.concatenate(z[:2], axis=1), jnp.concatenate(z[2:], axis=1)], axis=0
    )
    z = mm(z, doubled(rows, FLIP, c0, s0))
    v = mm(device_bits(mix, 1, FLIP), jnp.concatenate([z[:256], z[256:]], axis=1))
    v = [v[:, k * 128 : k * 128 + 128] for k in range(4)]
    for k in range(4):
        out[pl.ds(k, 256, stride=8), :] = v[k]
    lane = iota((128, 128), 1)
    upper, third = lane >= 64, bit(lane, 5) == 1
    for h in range(2):
        a = [v[k][h * 128 : h * 128 + 128].T for k in range(4)]
        a = [
            jnp.where(upper, pltpu.roll(a[2], 64, 1), a[0]),
            jnp.where(upper, pltpu.roll(a[3], 64, 1), a[1]),
            jnp.where(upper, a[2], pltpu.roll(a[0], 64, 1)),
            jnp.where(upper, a[3], pltpu.roll(a[1], 64, 1)),
        ]
        for k in (0, 2):
            low, high = a[k], a[k + 1]
            a[k] = jnp.where(third, pltpu.roll(high, 32, 1), low)
            a[k + 1] = jnp.where(third, high, pltpu.roll(low, 96, 1))
        for m in range(4):
            for q in range(4):
                at = (h * 4 + m) * 256 + 4 + q
                out[pl.ds(at, 32, stride=8), :] = a[m][q * 32 : q * 32 + 32]


def third_kernel(arrived, mix, final, marginal):
    c0, s0 = angle(mix, 1, 0)
    c2, s2 = angle(mix, 1, 2)
    small = table(
        (128, 128), [(k, k, FLIP, c0, s0) for k in range(6)] + [(6, 6, FLIP, c2, s2)]
    )
    w = doubled(small, FLIP, c2, s2)
    x = jnp.concatenate([arrived[pl.ds(k, 256, stride=8), :] for k in range(8)], axis=1)
    y = mm(w, x)
    own = own_pop()
    turns = [quarter_turns(own + k) for k in range(3)]
    for t in range(4):
        odd, sign = turns[bin(t).count("1")]
        f = []
        for c in range(2):
            part = [y[t * 64 : t * 64 + 64, (c * 2 + lb) * 128 : (c * 2 + lb) * 128 + 128] for lb in range(2)]
            f.append(jnp.concatenate(part, axis=0).T)
        re, im = jnp.where(odd, f[1], f[0]) * sign, jnp.where(odd, -f[0], f[1]) * sign
        for q in range(4):
            final[0, t, pl.ds(q, 32, stride=4), :] = re[q * 32 : q * 32 + 32]
            final[1, t, pl.ds(q, 32, stride=4), :] = im[q * 32 : q * 32 + 32]
    for q in range(4):
        chance = y[:, (4 + q) * 128 : (5 + q) * 128]
        chance = chance * chance
        chance = chance + pltpu.roll(chance, 64, 1)
        for t in range(4):
            turned = jnp.concatenate([chance[t * 64 : t * 64 + 64], chance[t * 64 : t * 64 + 64]], axis=0).T
            low = jnp.sum(turned[0:32], axis=0, keepdims=True)
            high = jnp.sum(turned[32:64], axis=0, keepdims=True)
            marginal[t, q : q + 1, :] = jnp.where(iota((1, 128), 1) >= 64, high, low) * (1.0 / 32.0)


def full(shape):
    return pl.BlockSpec(shape, lambda: (0,) * len(shape))


def call(body, outs, *args):
    specs = [
        pl.BlockSpec(memory_space=pltpu.SMEM) if a.shape == (2, 4) else full(a.shape) for a in args
    ]
    return pl.pallas_call(
        body,
        out_shape=[jax.ShapeDtypeStruct(s, jnp.float32) for s in outs],
        in_specs=specs,
        out_specs=[full(s) for s in outs],
    )(*args)


def exchange(values, *chunk):
    moved = lax.all_to_all(values.reshape(256, *chunk), GROUP, 0, 0, tiled=True)
    return moved.reshape(values.shape)


def on_device(amplitudes, energies, phase_angles, mix_angles):
    (sent,) = call(first_kernel, [(1536, 128)], amplitudes, energies, phase_angles, mix_angles)
    arrived = exchange(sent, 3, 2, 128)
    (sent,) = call(second_kernel, [(2048, 128)], arrived, mix_angles)
    arrived = exchange(sent, 8, 128)
    final, marginal = call(
        third_kernel, [(2, 4, 128, 128), (4, 4, 128)], arrived, mix_angles
    )
    return final, marginal


def solution(mesh):
    placed = (P(None, ("bank", "lane"), None, None), P(("bank", "lane"), None, None), P(), P())
    return jax.shard_map(
        on_device,
        mesh=mesh,
        in_specs=placed,
        out_specs=(P(None, ("bank", "lane"), None, None), P("lane", "bank", None)),
        check_vma=False,
    )
```

```python
import jax
import jax.numpy as jnp
from jax import lax
from jax.experimental import pallas as pl
from jax.experimental.pallas import tpu as pltpu
from jax.sharding import PartitionSpec as P


ROT, ROT_T, FLIP = 0, 1, 2
GROUP = ("lane", "bank")


def trig(x):
    y = x * x
    c = jnp.full_like(x, 1.0 / 20922789888000.0)
    s = jnp.full_like(x, 1.0 / 355687428096000.0)
    for k in (-87178291200.0, 479001600.0, -3628800.0, 40320.0, -720.0, 24.0, -2.0, 1.0):
        c = c * y + 1.0 / k
    for k in (-1307674368000.0, 6227020800.0, -39916800.0, 362880.0, -5040.0, 120.0, -6.0, 1.0):
        s = s * y + 1.0 / k
    return c, s * x


def angle(mix_ref, layer, group, width=128):
    return trig(jnp.full((1, width), mix_ref[layer, group], jnp.float32))


def iota(shape, dim):
    return lax.broadcasted_iota(jnp.int32, shape, dim)


def bit(value, k):
    return (value >> k) & 1


def pop(value, bits):
    total = bit(value, 0)
    for k in range(1, bits):
        total = total + bit(value, k)
    return total


def pair(kind, c, s):
    if kind == ROT:
        return c, s, -s, c
    if kind == ROT_T:
        return c, -s, s, c
    return c, s, s, -c


def table(shape, pairs):
    i, j = iota(shape, 0), iota(shape, 1)
    out = None
    for ki, kj, kind, c, s in pairs:
        a00, a01, a10, a11 = pair(kind, c, s)
        odd = bit(j, kj) == 1
        part = jnp.where(bit(i, ki) == 1, jnp.where(odd, a11, a10), jnp.where(odd, a01, a00))
        out = part if out is None else out * part
    return out


def doubled(small, kind, c, s):
    a00, a01, a10, a11 = pair(kind, c, s)
    top = jnp.concatenate([small * a00, small * a01], axis=1)
    low = jnp.concatenate([small * a10, small * a11], axis=1)
    return jnp.concatenate([top, low], axis=0)


def halves(x):
    high = x.astype(jnp.bfloat16)
    return high, (x - high.astype(jnp.float32)).astype(jnp.bfloat16)


def mm(a, b):
    ah, al = halves(a)
    bh, bl = halves(b)

    def one(p, q):
        return jnp.dot(p, q, preferred_element_type=jnp.float32)

    return one(ah, bh) + (one(ah, bl) + one(al, bh))


def own_pop():
    return pop(lax.axis_index("bank"), 5) + pop(lax.axis_index("lane"), 3)


def quarter_turns(extra):
    shape = (128, 128)
    p = pop(iota(shape, 0), 7) + pop(iota(shape, 1), 7) + extra
    return bit(p, 0) == 1, 1.0 - 2.0 * bit(p, 1).astype(jnp.float32)


def first_kernel(amp, en, ph, mix, out):
    own = own_pop()
    turns = [quarter_turns(own + k) for k in range(3)]
    xr, xi = [], []
    for t in range(4):
        odd, sign = turns[bin(t).count("1")]
        e = en[t]
        c, s = trig(ph[0:1, :] * e)
        c, s = jnp.where(odd, -s, c) * sign, jnp.where(odd, c, s) * sign
        re, im = amp[0, t], amp[1, t]
        xr.append(re * c + im * s)
        xi.append(im * c - re * s)
        e2 = (ph[1:2, :] * e).T
        for lb in range(2):
            out[pl.ds(t * 64 * 6 + 4 + lb, 64, stride=6), :] = e2[lb * 64 : lb * 64 + 64]
    c, s = angle(mix, 0, 2)
    x = []
    for v in (xr, xi):
        v = [c * v[0] + s * v[1], c * v[1] - s * v[0], c * v[2] + s * v[3], c * v[3] - s * v[2]]
        x += [c * v[0] + s * v[2], c * v[1] + s * v[3], c * v[2] - s * v[0], c * v[3] - s * v[1]]
    c, s = angle(mix, 0, 0)
    lanes = table((128, 128), [(k, k, ROT_T, c, s) for k in range(7)])
    c, s = angle(mix, 0, 1)
    rows = table((128, 128), [(k, k, ROT_T, c, s) for k in range(7)])
    y = mm(jnp.concatenate(x, axis=0), lanes)
    y = jnp.concatenate([y[k * 128 : k * 128 + 128].T for k in range(8)], axis=0)
    y = mm(y, rows)
    for c in range(2):
        for t in range(4):
            for lb in range(2):
                at = (c * 4 + t) * 128 + lb * 64
                out[pl.ds(t * 64 * 6 + c * 2 + lb, 64, stride=6), :] = y[at : at + 64]


def device_bits(mix, layer, kind):
    c2, s2 = angle(mix, layer, 2)
    c3, s3 = angle(mix, layer, 3)
    small = table(
        (128, 128), [(k, k, kind, c2, s2) for k in range(5)] + [(k, k, kind, c3, s3) for k in (5, 6)]
    )
    return doubled(small, kind, c3, s3)


def second_kernel(arrived, mix, out):
    x = jnp.concatenate([arrived[pl.ds(k, 256, stride=6), :] for k in range(4)], axis=1)
    y = mm(device_bits(mix, 0, ROT), x)
    z = [None] * 4
    for lb in range(2):
        c, s = trig(arrived[pl.ds(4 + lb, 256, stride=6), :])
        re, im = y[:, lb * 128 : lb * 128 + 128], y[:, 256 + lb * 128 : 384 + lb * 128]
        z[lb] = re * c + im * s
        z[2 + lb] = im * c - re * s
    c1, s1 = angle(mix, 1, 1)
    moved = (5, 6, 0, 1, 2, 3, 4)
    rows = table((128, 128), [(k, moved[k], FLIP, c1, s1) for k in range(7)])
    c0, s0 = angle(mix, 1, 0)
    z = jnp.concatenate(
        [jnp.concatenate(z[:2], axis=1), jnp.concatenate(z[2:], axis=1)], axis=0
    )
    z = mm(z, doubled(rows, FLIP, c0, s0))
    v = mm(device_bits(mix, 1, FLIP), jnp.concatenate([z[:256], z[256:]], axis=1))
    v = [v[:, k * 128 : k * 128 + 128] for k in range(4)]
    for k in range(4):
        out[pl.ds(k, 256, stride=8), :] = v[k]
    lane = iota((128, 128), 1)
    upper, third = lane >= 64, bit(lane, 5) == 1
    for h in range(2):
        a = [v[k][h * 128 : h * 128 + 128].T for k in range(4)]
        a = [
            jnp.where(upper, pltpu.roll(a[2], 64, 1), a[0]),
            jnp.where(upper, pltpu.roll(a[3], 64, 1), a[1]),
            jnp.where(upper, a[2], pltpu.roll(a[0], 64, 1)),
            jnp.where(upper, a[3], pltpu.roll(a[1], 64, 1)),
        ]
        for k in (0, 2):
            low, high = a[k], a[k + 1]
            a[k] = jnp.where(third, pltpu.roll(high, 32, 1), low)
            a[k + 1] = jnp.where(third, high, pltpu.roll(low, 96, 1))
        for m in range(4):
            for q in range(4):
                at = (h * 4 + m) * 256 + 4 + q
                out[pl.ds(at, 32, stride=8), :] = a[m][q * 32 : q * 32 + 32]


def third_kernel(arrived, mix, final, marginal):
    c0, s0 = angle(mix, 1, 0)
    c2, s2 = angle(mix, 1, 2)
    small = table(
        (128, 128), [(k, k, FLIP, c0, s0) for k in range(6)] + [(6, 6, FLIP, c2, s2)]
    )
    w = doubled(small, FLIP, c2, s2)
    x = jnp.concatenate([arrived[pl.ds(k, 256, stride=8), :] for k in range(8)], axis=1)
    y = mm(w, x)
    own = own_pop()
    turns = [quarter_turns(own + k) for k in range(3)]
    for t in range(4):
        odd, sign = turns[bin(t).count("1")]
        f = []
        for c in range(2):
            part = [y[t * 64 : t * 64 + 64, (c * 2 + lb) * 128 : (c * 2 + lb) * 128 + 128] for lb in range(2)]
            f.append(jnp.concatenate(part, axis=0).T)
        re, im = jnp.where(odd, f[1], f[0]) * sign, jnp.where(odd, -f[0], f[1]) * sign
        for q in range(4):
            final[0, t, pl.ds(q, 32, stride=4), :] = re[q * 32 : q * 32 + 32]
            final[1, t, pl.ds(q, 32, stride=4), :] = im[q * 32 : q * 32 + 32]
    for q in range(4):
        chance = y[:, (4 + q) * 128 : (5 + q) * 128]
        chance = chance * chance
        chance = chance + pltpu.roll(chance, 64, 1)
        for t in range(4):
            turned = jnp.concatenate([chance[t * 64 : t * 64 + 64], chance[t * 64 : t * 64 + 64]], axis=0).T
            low = jnp.sum(turned[0:32], axis=0, keepdims=True)
            high = jnp.sum(turned[32:64], axis=0, keepdims=True)
            marginal[t, q : q + 1, :] = jnp.where(iota((1, 128), 1) >= 64, high, low) * (1.0 / 32.0)


def full(shape):
    return pl.BlockSpec(shape, lambda: (0,) * len(shape))


def call(body, outs, *args, inner=False):
    specs = [
        pl.BlockSpec(memory_space=pltpu.SMEM) if a.shape == (2, 4) else pl.BlockSpec(memory_space=pltpu.VMEM) if a.shape[0] > 1000 else full(a.shape) for a in args
    ]
    return pl.pallas_call(
        body,
        out_shape=[
            pltpu.VMEM(s, jnp.float32) if inner else jax.ShapeDtypeStruct(s, jnp.float32) for s in outs
        ],
        in_specs=specs,
        out_specs=[
            pl.BlockSpec(memory_space=pltpu.VMEM) if inner else full(s) for s in outs
        ],
    )(*args)


def exchange(values, *chunk):
    moved = lax.all_to_all(values.reshape(256, *chunk), GROUP, 0, 0, tiled=True)
    return pltpu.with_memory_space_constraint(moved.reshape(values.shape), pltpu.VMEM)


def on_device(amplitudes, energies, phase_angles, mix_angles):
    (sent,) = call(first_kernel, [(1536, 128)], amplitudes, energies, phase_angles, mix_angles, inner=True)
    arrived = exchange(sent, 3, 2, 128)
    (sent,) = call(second_kernel, [(2048, 128)], arrived, mix_angles, inner=True)
    arrived = exchange(sent, 8, 128)
    final, marginal = call(
        third_kernel, [(2, 4, 128, 128), (4, 4, 128)], arrived, mix_angles
    )
    return final, marginal


def solution(mesh):
    placed = (P(None, ("bank", "lane"), None, None), P(("bank", "lane"), None, None), P(), P())
    return jax.shard_map(
        on_device,
        mesh=mesh,
        in_specs=placed,
        out_specs=(P(None, ("bank", "lane"), None, None), P("lane", "bank", None)),
        check_vma=False,
    )
```

```python
import jax
import jax.numpy as jnp
from jax import lax
from jax.experimental import pallas as pl
from jax.experimental.pallas import tpu as pltpu
from jax.sharding import PartitionSpec as P


ROT, ROT_T, FLIP = 0, 1, 2
GROUP = ("lane", "bank")


def trig(x):
    h = x * 0.5
    y = h * h
    c = jnp.full_like(x, 1.0 / 479001600.0)
    s = jnp.full_like(x, 1.0 / 6227020800.0)
    for k in (-3628800.0, 40320.0, -720.0, 24.0, -2.0):
        c = c * y + 1.0 / k
    for k in (-39916800.0, 362880.0, -5040.0, 120.0, -6.0, 1.0):
        s = s * y + 1.0 / k
    s = s * h
    c = c * y
    return 1.0 - 2.0 * s * s, 2.0 * s + 2.0 * s * c


def angle(mix_ref, layer, group, width=128):
    return trig(jnp.full((1, width), mix_ref[layer, group], jnp.float32))


def iota(shape, dim):
    return lax.broadcasted_iota(jnp.int32, shape, dim)


def bit(value, k):
    return (value >> k) & 1


def pop(value, bits):
    total = bit(value, 0)
    for k in range(1, bits):
        total = total + bit(value, k)
    return total


def pair(kind, c, s):
    if kind == ROT:
        return c, s, -s, c
    if kind == ROT_T:
        return c, -s, s, c
    return c, s, s, -c


def table(pairs):
    j = iota((1, 128), 1)
    i = iota((8, 1), 0)
    out = jnp.ones((8, 128), jnp.float32)
    for k, kj, kind, c, s in pairs:
        a00, a01, a10, a11 = pair(kind, c, s)
        odd = bit(j, kj) == 1
        upper, lower = jnp.where(odd, a01, a00), jnp.where(odd, a11, a10)
        if k < 3:
            out = out * jnp.where(bit(i, k) == 1, lower, upper)
        else:
            out = jnp.concatenate([out * upper, out * lower], axis=0)
    return out


def doubled(small, kind, c, s):
    a00, a01, a10, a11 = pair(kind, c, s)
    top = jnp.concatenate([small * a00, small * a01], axis=1)
    low = jnp.concatenate([small * a10, small * a11], axis=1)
    return jnp.concatenate([top, low], axis=0)


def halves(x):
    high = x.astype(jnp.bfloat16)
    return high, (x - high.astype(jnp.float32)).astype(jnp.bfloat16)


def mm(a, b):
    ah, al = halves(a)
    bh, bl = halves(b)
    return jnp.dot(
        jnp.concatenate([ah, ah, al], axis=1),
        jnp.concatenate([bh, bl, bh], axis=0),
        preferred_element_type=jnp.float32,
    )


def own_pop():
    return pop(lax.axis_index("bank"), 5) + pop(lax.axis_index("lane"), 3)


def quarter_turns(extra):
    shape = (128, 128)
    p = pop(iota(shape, 0), 7) + pop(iota(shape, 1), 7) + extra
    return bit(p, 0) == 1, 1.0 - 2.0 * bit(p, 1).astype(jnp.float32)


def first_kernel(amp, en, ph, mix, out):
    own = own_pop()
    turns = [quarter_turns(own + k) for k in range(3)]
    xr, xi = [], []
    for t in range(4):
        odd, sign = turns[bin(t).count("1")]
        e = en[t]
        c, s = trig(ph[0:1, :] * e)
        c, s = jnp.where(odd, -s, c) * sign, jnp.where(odd, c, s) * sign
        re, im = amp[0, t], amp[1, t]
        xr.append(re * c + im * s)
        xi.append(im * c - re * s)
        e2 = (ph[1:2, :] * e).T
        for lb in range(2):
            out[pl.ds(t * 64 * 6 + 4 + lb, 64, stride=6), :] = e2[lb * 64 : lb * 64 + 64]
    bits = range(7)
    c2, s2 = angle(mix, 0, 2)
    c, s = angle(mix, 0, 0)
    lanes = doubled(table([(k, k, ROT_T, c, s) for k in bits]), ROT_T, c2, s2)
    c, s = angle(mix, 0, 1)
    rows = doubled(table([(k, k, ROT_T, c, s) for k in bits]), ROT_T, c2, s2)
    x = [jnp.concatenate([v[t], v[t + 1]], axis=1) for v in (xr, xi) for t in (0, 2)]
    y = mm(jnp.concatenate(x, axis=0), lanes)
    z = []
    for c in range(2):
        for low in range(2):
            part = [
                y[(c * 2 + high) * 128 : (c * 2 + high) * 128 + 128, low * 128 : low * 128 + 128].T
                for high in range(2)
            ]
            z.append(jnp.concatenate(part, axis=1))
    y = mm(jnp.concatenate(z, axis=0), rows)
    for c in range(2):
        for t in range(4):
            for lb in range(2):
                at = (c * 2 + t % 2) * 128 + lb * 64
                out[pl.ds(t * 64 * 6 + c * 2 + lb, 64, stride=6), :] = y[at : at + 64, t // 2 * 128 : t // 2 * 128 + 128]


def device_bits(mix, layer, kind):
    c2, s2 = angle(mix, layer, 2)
    c3, s3 = angle(mix, layer, 3)
    small = table([(k, k, kind, c2, s2) for k in range(5)] + [(k, k, kind, c3, s3) for k in (5, 6)])
    return doubled(small, kind, c3, s3)


def second_kernel(arrived, mix, out):
    x = jnp.concatenate([arrived[pl.ds(k, 256, stride=6), :] for k in range(4)], axis=1)
    y = mm(device_bits(mix, 0, ROT), x)
    z = [None] * 4
    for lb in range(2):
        c, s = trig(arrived[pl.ds(4 + lb, 256, stride=6), :])
        re, im = y[:, lb * 128 : lb * 128 + 128], y[:, 256 + lb * 128 : 384 + lb * 128]
        z[lb] = re * c + im * s
        z[2 + lb] = im * c - re * s
    c1, s1 = angle(mix, 1, 1)
    moved = (5, 6, 0, 1, 2, 3, 4)
    rows = table([(k, moved[k], FLIP, c1, s1) for k in range(7)])
    c0, s0 = angle(mix, 1, 0)
    z = jnp.concatenate(
        [jnp.concatenate(z[:2], axis=1), jnp.concatenate(z[2:], axis=1)], axis=0
    )
    z = mm(z, doubled(rows, FLIP, c0, s0))
    v = mm(device_bits(mix, 1, FLIP), jnp.concatenate([z[:256], z[256:]], axis=1))
    v = [v[:, k * 128 : k * 128 + 128] for k in range(4)]
    for k in range(4):
        out[pl.ds(k, 256, stride=8), :] = v[k]
    for m in range(8):
        a = jnp.concatenate([v[k][m * 32 : m * 32 + 32] for k in range(4)], axis=0).T
        for q in range(4):
            out[pl.ds(m * 256 + 4 + q, 32, stride=8), :] = a[q * 32 : q * 32 + 32]


def third_kernel(arrived, mix, final, marginal):
    c0, s0 = angle(mix, 1, 0)
    c2, s2 = angle(mix, 1, 2)
    small = table([(k, k, FLIP, c0, s0) for k in range(6)] + [(6, 6, FLIP, c2, s2)])
    w = doubled(small, FLIP, c2, s2)
    x = jnp.concatenate([arrived[pl.ds(k, 256, stride=8), :] for k in range(8)], axis=1)
    y = mm(w, x)
    own = own_pop()
    turns = [quarter_turns(own + k) for k in range(3)]
    for t in range(4):
        odd, sign = turns[bin(t).count("1")]
        f = []
        for c in range(2):
            part = [y[t * 64 : t * 64 + 64, (c * 2 + lb) * 128 : (c * 2 + lb) * 128 + 128] for lb in range(2)]
            f.append(jnp.concatenate(part, axis=0).T)
        re, im = jnp.where(odd, f[1], f[0]) * sign, jnp.where(odd, -f[0], f[1]) * sign
        for q in range(4):
            final[0, t, pl.ds(q, 32, stride=4), :] = re[q * 32 : q * 32 + 32]
            final[1, t, pl.ds(q, 32, stride=4), :] = im[q * 32 : q * 32 + 32]
    pick = jnp.where(bit(iota((8, 128), 1), 5) == iota((8, 128), 0), 1.0 / 32.0, 0.0).astype(jnp.bfloat16)
    upper = iota((1, 128), 1) >= 64
    for q in range(4):
        chance = y[:, (4 + q) * 128 : (5 + q) * 128]
        high, low = halves(chance * chance)
        total = lax.dot_general(
            jnp.concatenate([pick, pick], axis=1),
            jnp.concatenate([high, low], axis=1),
            (((1,), (1,)), ((), ())),
            preferred_element_type=jnp.float32,
        )
        for t in range(4):
            part = total[:, t // 2 * 128 : t // 2 * 128 + 128]
            moved = pltpu.roll(part, 64, 1)
            first, second = (moved, part) if t % 2 else (part, moved)
            marginal[t, q : q + 1, :] = jnp.where(upper, second[1:2], first[0:1])


def full(shape):
    return pl.BlockSpec(shape, lambda: (0,) * len(shape))


def call(body, outs, *args, inner=False):
    specs = [
        pl.BlockSpec(memory_space=pltpu.SMEM) if a.shape == (2, 4) else pl.BlockSpec(memory_space=pltpu.VMEM) if a.shape[0] > 1000 else full(a.shape) for a in args
    ]
    return pl.pallas_call(
        body,
        out_shape=[
            pltpu.VMEM(s, jnp.float32) if inner else jax.ShapeDtypeStruct(s, jnp.float32) for s in outs
        ],
        in_specs=specs,
        out_specs=[
            pl.BlockSpec(memory_space=pltpu.VMEM) if inner else full(s) for s in outs
        ],
    )(*args)


def exchange(values, *chunk):
    moved = lax.all_to_all(values.reshape(256, *chunk), GROUP, 0, 0, tiled=True)
    return pltpu.with_memory_space_constraint(moved.reshape(values.shape), pltpu.VMEM)


def on_device(amplitudes, energies, phase_angles, mix_angles):
    (sent,) = call(first_kernel, [(1536, 128)], amplitudes, energies, phase_angles, mix_angles, inner=True)
    arrived = exchange(sent, 3, 2, 128)
    (sent,) = call(second_kernel, [(2048, 128)], arrived, mix_angles, inner=True)
    arrived = exchange(sent, 8, 128)
    final, marginal = call(
        third_kernel, [(2, 4, 128, 128), (4, 4, 128)], arrived, mix_angles
    )
    return final, marginal


def solution(mesh):
    placed = (P(None, ("bank", "lane"), None, None), P(("bank", "lane"), None, None), P(), P())
    return jax.shard_map(
        on_device,
        mesh=mesh,
        in_specs=placed,
        out_specs=(P(None, ("bank", "lane"), None, None), P("lane", "bank", None)),
        check_vma=False,
    )
```

```python
import jax
import jax.numpy as jnp
from jax import lax
from jax.experimental import pallas as pl
from jax.experimental.pallas import tpu as pltpu
from jax.sharding import PartitionSpec as P


ROT, ROT_T, FLIP = 0, 1, 2
GROUP = ("lane", "bank")


def trig(x):
    h = x * 0.5
    y = h * h
    c = jnp.full_like(x, 1.0 / 479001600.0)
    s = jnp.full_like(x, 1.0 / 6227020800.0)
    for k in (-3628800.0, 40320.0, -720.0, 24.0, -2.0):
        c = c * y + 1.0 / k
    for k in (-39916800.0, 362880.0, -5040.0, 120.0, -6.0, 1.0):
        s = s * y + 1.0 / k
    s = s * h
    c = c * y
    return 1.0 - 2.0 * s * s, 2.0 * s + 2.0 * s * c


def angle(turns, layer, group):
    k = layer * 4 + group
    return turns[k : k + 1, :], turns[8 + k : 9 + k, :]


def iota(shape, dim):
    return lax.broadcasted_iota(jnp.int32, shape, dim)


def bit(value, k):
    return (value >> k) & 1


def pop(value, bits):
    total = bit(value, 0)
    for k in range(1, bits):
        total = total + bit(value, k)
    return total


def pair(kind, c, s):
    if kind == ROT:
        return c, s, -s, c
    if kind == ROT_T:
        return c, -s, s, c
    return c, s, s, -c


def table(pairs):
    j = iota((1, 128), 1)
    i = iota((8, 1), 0)
    out = jnp.ones((8, 128), jnp.float32)
    for k, kj, kind, c, s in pairs:
        a00, a01, a10, a11 = pair(kind, c, s)
        odd = bit(j, kj) == 1
        upper, lower = jnp.where(odd, a01, a00), jnp.where(odd, a11, a10)
        if k < 3:
            out = out * jnp.where(bit(i, k) == 1, lower, upper)
        else:
            out = jnp.concatenate([out * upper, out * lower], axis=0)
    return out


def doubled(small, kind, c, s):
    a00, a01, a10, a11 = pair(kind, c, s)
    top = jnp.concatenate([small * a00, small * a01], axis=1)
    low = jnp.concatenate([small * a10, small * a11], axis=1)
    return jnp.concatenate([top, low], axis=0)


def halves(x):
    high = x.astype(jnp.bfloat16)
    return high, (x - high.astype(jnp.float32)).astype(jnp.bfloat16)


def mm(a, b):
    ah, al = halves(a)
    bh, bl = halves(b)
    return jnp.dot(
        jnp.concatenate([ah, ah, al], axis=1),
        jnp.concatenate([bh, bl, bh], axis=0),
        preferred_element_type=jnp.float32,
    )


def own_pop():
    return pop(lax.axis_index("bank"), 5) + pop(lax.axis_index("lane"), 3)


def quarter_turns(extra):
    shape = (128, 128)
    p = pop(iota(shape, 0), 7) + pop(iota(shape, 1), 7) + extra
    return bit(p, 0) == 1, 1.0 - 2.0 * bit(p, 1).astype(jnp.float32)


def first_kernel(amp_in, en_in, ph_in, mix_in, out, turns, amp, en, ph, mix, sems):
    copies = [(mix_in, mix), (ph_in, ph), (en_in, en), (amp_in, amp)]
    copies = [pltpu.make_async_copy(a, b, sems.at[k]) for k, (a, b) in enumerate(copies)]
    for copy in copies:
        copy.start()
    own = own_pop()
    quarters = [quarter_turns(own + k) for k in range(3)]
    for copy in copies:
        copy.wait()
    xr, xi = [], []
    for t in range(4):
        odd, sign = quarters[bin(t).count("1")]
        e = en[t]
        c, s = trig(ph[0:1, :] * e)
        c, s = jnp.where(odd, -s, c) * sign, jnp.where(odd, c, s) * sign
        re, im = amp[0, t], amp[1, t]
        xr.append(re * c + im * s)
        xi.append(im * c - re * s)
        e2 = (ph[1:2, :] * e).T
        for lb in range(2):
            out[pl.ds(t * 64 * 6 + 4 + lb, 64, stride=6), :] = e2[lb * 64 : lb * 64 + 64]
    row = iota((8, 128), 0)
    b = jnp.zeros((8, 128), jnp.float32)
    for k in range(8):
        b = jnp.where(row == k, mix[k // 4, k % 4], b)
    c, s = trig(b)
    turns[0:8, :] = c
    turns[8:16, :] = s
    bits = range(7)
    c2, s2 = angle(turns, 0, 2)
    c, s = angle(turns, 0, 0)
    lanes = doubled(table([(k, k, ROT_T, c, s) for k in bits]), ROT_T, c2, s2)
    c, s = angle(turns, 0, 1)
    rows = doubled(table([(k, k, ROT_T, c, s) for k in bits]), ROT_T, c2, s2)
    x = [jnp.concatenate([v[t], v[t + 1]], axis=1) for v in (xr, xi) for t in (0, 2)]
    y = mm(jnp.concatenate(x, axis=0), lanes)
    z = []
    for c in range(2):
        for low in range(2):
            part = [
                y[(c * 2 + high) * 128 : (c * 2 + high) * 128 + 128, low * 128 : low * 128 + 128].T
                for high in range(2)
            ]
            z.append(jnp.concatenate(part, axis=1))
    y = mm(jnp.concatenate(z, axis=0), rows)
    for c in range(2):
        for t in range(4):
            for lb in range(2):
                at = (c * 2 + t % 2) * 128 + lb * 64
                out[pl.ds(t * 64 * 6 + c * 2 + lb, 64, stride=6), :] = y[at : at + 64, t // 2 * 128 : t // 2 * 128 + 128]


def device_bits(turns, layer, kind):
    c2, s2 = angle(turns, layer, 2)
    c3, s3 = angle(turns, layer, 3)
    small = table([(k, k, kind, c2, s2) for k in range(5)] + [(k, k, kind, c3, s3) for k in (5, 6)])
    return doubled(small, kind, c3, s3)


def second_kernel(arrived, turns, out):
    x = jnp.concatenate([arrived[pl.ds(k, 256, stride=6), :] for k in range(4)], axis=1)
    y = mm(device_bits(turns, 0, ROT), x)
    z = [None] * 4
    for lb in range(2):
        c, s = trig(arrived[pl.ds(4 + lb, 256, stride=6), :])
        re, im = y[:, lb * 128 : lb * 128 + 128], y[:, 256 + lb * 128 : 384 + lb * 128]
        z[lb] = re * c + im * s
        z[2 + lb] = im * c - re * s
    c1, s1 = angle(turns, 1, 1)
    moved = (5, 6, 0, 1, 2, 3, 4)
    rows = table([(k, moved[k], FLIP, c1, s1) for k in range(7)])
    c0, s0 = angle(turns, 1, 0)
    z = jnp.concatenate(
        [jnp.concatenate(z[:2], axis=1), jnp.concatenate(z[2:], axis=1)], axis=0
    )
    z = mm(z, doubled(rows, FLIP, c0, s0))
    v = mm(device_bits(turns, 1, FLIP), jnp.concatenate([z[:256], z[256:]], axis=1))
    v = [v[:, k * 128 : k * 128 + 128] for k in range(4)]
    for k in range(4):
        out[pl.ds(k, 256, stride=8), :] = v[k]
    for m in range(8):
        a = jnp.concatenate([v[k][m * 32 : m * 32 + 32] for k in range(4)], axis=0).T
        for q in range(4):
            out[pl.ds(m * 256 + 4 + q, 32, stride=8), :] = a[q * 32 : q * 32 + 32]


def third_kernel(arrived, turns, final_out, marginal_out, final, marginal, sems):
    c0, s0 = angle(turns, 1, 0)
    c2, s2 = angle(turns, 1, 2)
    small = table([(k, k, FLIP, c0, s0) for k in range(6)] + [(6, 6, FLIP, c2, s2)])
    w = doubled(small, FLIP, c2, s2)
    y = mm(w, jnp.concatenate([arrived[pl.ds(k, 256, stride=8), :] for k in range(4)], axis=1))
    own = own_pop()
    quarters = [quarter_turns(own + k) for k in range(3)]
    copies = []
    for t in range(4):
        odd, sign = quarters[bin(t).count("1")]
        f = []
        for c in range(2):
            part = [y[t * 64 : t * 64 + 64, (c * 2 + lb) * 128 : (c * 2 + lb) * 128 + 128] for lb in range(2)]
            f.append(jnp.concatenate(part, axis=0).T)
        re, im = jnp.where(odd, f[1], f[0]) * sign, jnp.where(odd, -f[0], f[1]) * sign
        for q in range(4):
            final[0, t, pl.ds(q, 32, stride=4), :] = re[q * 32 : q * 32 + 32]
            final[1, t, pl.ds(q, 32, stride=4), :] = im[q * 32 : q * 32 + 32]
        copies.append(pltpu.make_async_copy(final.at[:, t], final_out.at[:, t], sems.at[t]))
        copies[t].start()
    y = mm(w, jnp.concatenate([arrived[pl.ds(4 + k, 256, stride=8), :] for k in range(4)], axis=1))
    pick = jnp.where(bit(iota((8, 128), 1), 5) == iota((8, 128), 0), 1.0 / 32.0, 0.0).astype(jnp.bfloat16)
    upper = iota((1, 128), 1) >= 64
    for q in range(4):
        chance = y[:, q * 128 : q * 128 + 128]
        high, low = halves(chance * chance)
        total = lax.dot_general(
            jnp.concatenate([pick, pick], axis=1),
            jnp.concatenate([high, low], axis=1),
            (((1,), (1,)), ((), ())),
            preferred_element_type=jnp.float32,
        )
        for t in range(4):
            part = total[:, t // 2 * 128 : t // 2 * 128 + 128]
            moved = pltpu.roll(part, 64, 1)
            first, second = (moved, part) if t % 2 else (part, moved)
            marginal[t, q : q + 1, :] = jnp.where(upper, second[1:2], first[0:1])
    copies.append(pltpu.make_async_copy(marginal, marginal_out, sems.at[4]))
    copies[4].start()
    for copy in copies:
        copy.wait()


HERE, AWAY = pl.BlockSpec(memory_space=pltpu.VMEM), pl.BlockSpec(memory_space=pl.ANY)


def inner(*shape):
    return pltpu.VMEM(shape, jnp.float32)


def kept(value):
    return pltpu.with_memory_space_constraint(value, pltpu.VMEM)


def exchange(values, *chunk):
    moved = lax.all_to_all(values.reshape(256, *chunk), GROUP, 0, 0, tiled=True)
    return kept(moved.reshape(values.shape))


def on_device(amplitudes, energies, phase_angles, mix_angles):
    sent, turns = pl.pallas_call(
        first_kernel,
        out_shape=[inner(1536, 128), inner(16, 128)],
        in_specs=[AWAY] * 4,
        out_specs=[HERE, HERE],
        scratch_shapes=[
            inner(2, 4, 128, 128),
            inner(4, 128, 128),
            inner(2, 128),
            pltpu.SMEM((2, 4), jnp.float32),
            pltpu.SemaphoreType.DMA((4,)),
        ],
    )(amplitudes, energies, phase_angles, mix_angles)
    turns = kept(turns)
    arrived = exchange(sent, 3, 2, 128)
    sent = pl.pallas_call(
        second_kernel, out_shape=inner(2048, 128), in_specs=[HERE, HERE], out_specs=HERE
    )(arrived, turns)
    arrived = exchange(sent, 8, 128)
    return pl.pallas_call(
        third_kernel,
        out_shape=[
            jax.ShapeDtypeStruct((2, 4, 128, 128), jnp.float32),
            jax.ShapeDtypeStruct((4, 4, 128), jnp.float32),
        ],
        in_specs=[HERE, HERE],
        out_specs=[AWAY, AWAY],
        scratch_shapes=[inner(2, 4, 128, 128), inner(4, 4, 128), pltpu.SemaphoreType.DMA((5,))],
    )(arrived, turns)


def solution(mesh):
    placed = (P(None, ("bank", "lane"), None, None), P(("bank", "lane"), None, None), P(), P())
    return jax.shard_map(
        on_device,
        mesh=mesh,
        in_specs=placed,
        out_specs=(P(None, ("bank", "lane"), None, None), P("lane", "bank", None)),
        check_vma=False,
    )
```

```python
import jax
import jax.numpy as jnp
from jax import lax
from jax.experimental import pallas as pl
from jax.experimental.pallas import tpu as pltpu
from jax.sharding import Mesh, PartitionSpec as P


ROT, ROT_T, FLIP = 0, 1, 2
AXES = ("zh", "y", "x", "zl", "core")
GROUP = ("zh", "zl", "y", "x", "core")


def trig(x):
    h = x * 0.5
    y = h * h
    c = jnp.full_like(x, 1.0 / 479001600.0)
    s = jnp.full_like(x, 1.0 / 6227020800.0)
    for k in (-3628800.0, 40320.0, -720.0, 24.0, -2.0):
        c = c * y + 1.0 / k
    for k in (-39916800.0, 362880.0, -5040.0, 120.0, -6.0, 1.0):
        s = s * y + 1.0 / k
    s = s * h
    c = c * y
    return 1.0 - 2.0 * s * s, 2.0 * s + 2.0 * s * c


def angle(turns, layer, group):
    k = layer * 4 + group
    return turns[k : k + 1, :], turns[8 + k : 9 + k, :]


def iota(shape, dim):
    return lax.broadcasted_iota(jnp.int32, shape, dim)


def bit(value, k):
    return (value >> k) & 1


def pop(value, bits):
    total = bit(value, 0)
    for k in range(1, bits):
        total = total + bit(value, k)
    return total


def pair(kind, c, s):
    if kind == ROT:
        return c, s, -s, c
    if kind == ROT_T:
        return c, -s, s, c
    return c, s, s, -c


def table(pairs, width=128):
    j = iota((1, width), 1)
    i = iota((8, 1), 0)
    out = jnp.ones((8, width), jnp.float32)
    for k, kj, kind, c, s in pairs:
        if width > 128:
            c, s = jnp.concatenate([c, c], axis=1), jnp.concatenate([s, s], axis=1)
        a00, a01, a10, a11 = pair(kind, c, s)
        odd = bit(j, kj) == 1
        upper, lower = jnp.where(odd, a01, a00), jnp.where(odd, a11, a10)
        if k < 3:
            out = out * jnp.where(bit(i, k) == 1, lower, upper)
        else:
            out = jnp.concatenate([out * upper, out * lower], axis=0)
    return out


def doubled(small, kind, c, s):
    a00, a01, a10, a11 = pair(kind, c, s)
    top = jnp.concatenate([small * a00, small * a01], axis=1)
    low = jnp.concatenate([small * a10, small * a11], axis=1)
    return jnp.concatenate([top, low], axis=0)


def halves(x):
    high = x.astype(jnp.bfloat16)
    return high, (x - high.astype(jnp.float32)).astype(jnp.bfloat16)


def mm(a, b):
    ah, al = halves(a)
    bh, bl = halves(b)
    return jnp.dot(
        jnp.concatenate([ah, ah, al], axis=1),
        jnp.concatenate([bh, bl, bh], axis=0),
        preferred_element_type=jnp.float32,
    )


def own_pop():
    return sum(pop(lax.axis_index(axis), 1 if axis in ("zh", "core") else 2) for axis in AXES)


def quarter_turns(extra):
    shape = (128, 128)
    p = pop(iota(shape, 0), 7) + pop(iota(shape, 1), 7) + extra
    return bit(p, 0) == 1, 1.0 - 2.0 * bit(p, 1).astype(jnp.float32)


def first_kernel(amp_in, en_in, ph_in, mix_in, out, turns, amp, en, ph, mix, sems):
    copies = [(mix_in, mix), (ph_in, ph), (en_in, en), (amp_in, amp)]
    copies = [pltpu.make_async_copy(a, b, sems.at[k]) for k, (a, b) in enumerate(copies)]
    for copy in copies:
        copy.start()
    own = own_pop()
    quarters = [quarter_turns(own + k) for k in range(3)]
    for copy in copies:
        copy.wait()
    xr, xi = [], []
    for t in range(4):
        odd, sign = quarters[bin(t).count("1")]
        e = en[t]
        c, s = trig(ph[0:1, :] * e)
        c, s = jnp.where(odd, -s, c) * sign, jnp.where(odd, c, s) * sign
        re, im = amp[0, t], amp[1, t]
        xr.append(re * c + im * s)
        xi.append(im * c - re * s)
        e2 = (ph[1:2, :] * e).T
        for lb in range(2):
            out[pl.ds(t * 64 * 6 + 4 + lb, 64, stride=6), :] = e2[lb * 64 : lb * 64 + 64]
    row = iota((8, 128), 0)
    b = jnp.zeros((8, 128), jnp.float32)
    for k in range(8):
        b = jnp.where(row == k, mix[k // 4, k % 4], b)
    c, s = trig(b)
    turns[0:8, :] = c
    turns[8:16, :] = s
    bits = range(7)
    c2, s2 = angle(turns, 0, 2)
    c, s = angle(turns, 0, 0)
    lanes = doubled(table([(k, k, ROT_T, c, s) for k in bits]), ROT_T, c2, s2)
    c, s = angle(turns, 0, 1)
    rows = doubled(table([(k, k, ROT_T, c, s) for k in bits]), ROT_T, c2, s2)
    x = [jnp.concatenate([v[t], v[t + 1]], axis=1) for v in (xr, xi) for t in (0, 2)]
    y = mm(jnp.concatenate(x, axis=0), lanes)
    z = []
    for c in range(2):
        for low in range(2):
            part = [
                y[(c * 2 + high) * 128 : (c * 2 + high) * 128 + 128, low * 128 : low * 128 + 128].T
                for high in range(2)
            ]
            z.append(jnp.concatenate(part, axis=1))
    y = mm(jnp.concatenate(z, axis=0), rows)
    for c in range(2):
        for t in range(4):
            for lb in range(2):
                at = (c * 2 + t % 2) * 128 + lb * 64
                out[pl.ds(t * 64 * 6 + c * 2 + lb, 64, stride=6), :] = y[at : at + 64, t // 2 * 128 : t // 2 * 128 + 128]


MIDDLE = (0, 5, 6)
SORTED = (1, 2, 3, 4, 7, 0, 5, 6)


def device_bits(turns, layer, kind, order):
    return table([(k, kj, kind, *angle(turns, layer, 3 if kj in MIDDLE else 2)) for k, kj in enumerate(order)], 256)


def second_kernel(arrived, turns, out):
    x = jnp.concatenate([arrived[pl.ds(k, 256, stride=6), :] for k in range(4)], axis=1)
    y = mm(device_bits(turns, 0, ROT, range(8)), x)
    z = [None] * 4
    for lb in range(2):
        c, s = trig(arrived[pl.ds(4 + lb, 256, stride=6), :])
        re, im = y[:, lb * 128 : lb * 128 + 128], y[:, 256 + lb * 128 : 384 + lb * 128]
        z[lb] = re * c + im * s
        z[2 + lb] = im * c - re * s
    c1, s1 = angle(turns, 1, 1)
    moved = (5, 6, 0, 1, 2, 3, 4)
    rows = table([(k, moved[k], FLIP, c1, s1) for k in range(7)])
    c0, s0 = angle(turns, 1, 0)
    z = jnp.concatenate(
        [jnp.concatenate(z[:2], axis=1), jnp.concatenate(z[2:], axis=1)], axis=0
    )
    z = mm(z, doubled(rows, FLIP, c0, s0))
    v = mm(device_bits(turns, 1, FLIP, SORTED), jnp.concatenate([z[:256], z[256:]], axis=1))
    v = [v[:, k * 128 : k * 128 + 128] for k in range(4)]
    for m in range(8):
        to = [(zh * 128 + (m // 2) * 32 + m % 2) * 8 for zh in range(2)]
        for k in range(4):
            for zh in range(2):
                at = m * 32 + zh * 16
                out[pl.ds(to[zh] + k, 16, stride=16), :] = v[k][at : at + 16]
        a = jnp.concatenate([v[k][m * 32 : m * 32 + 32] for k in range(4)], axis=0).T
        for q in range(4):
            for zh in range(2):
                at = q * 32 + zh * 16
                out[pl.ds(to[zh] + 4 + q, 16, stride=16), :] = a[at : at + 16]


def third_kernel(arrived, turns, final_out, marginal_out, final, marginal, sems):
    c0, s0 = angle(turns, 1, 0)
    c2, s2 = angle(turns, 1, 2)
    small = table([(k, k, FLIP, c0, s0) for k in range(6)] + [(6, 6, FLIP, c2, s2)])
    w = doubled(small, FLIP, c2, s2)
    y = mm(w, jnp.concatenate([arrived[pl.ds(k, 256, stride=8), :] for k in range(4)], axis=1))
    own = own_pop()
    quarters = [quarter_turns(own + k) for k in range(3)]
    copies = []
    for t in range(4):
        odd, sign = quarters[bin(t).count("1")]
        f = []
        for c in range(2):
            part = [y[t * 64 : t * 64 + 64, (c * 2 + lb) * 128 : (c * 2 + lb) * 128 + 128] for lb in range(2)]
            f.append(jnp.concatenate(part, axis=0).T)
        re, im = jnp.where(odd, f[1], f[0]) * sign, jnp.where(odd, -f[0], f[1]) * sign
        for q in range(4):
            final[0, t, pl.ds(q, 32, stride=4), :] = re[q * 32 : q * 32 + 32]
            final[1, t, pl.ds(q, 32, stride=4), :] = im[q * 32 : q * 32 + 32]
        copies.append(pltpu.make_async_copy(final.at[:, t], final_out.at[:, t], sems.at[t]))
        copies[t].start()
    y = mm(w, jnp.concatenate([arrived[pl.ds(4 + k, 256, stride=8), :] for k in range(4)], axis=1))
    pick = jnp.where(bit(iota((8, 128), 1), 5) == iota((8, 128), 0), 1.0 / 32.0, 0.0).astype(jnp.bfloat16)
    upper = iota((1, 128), 1) >= 64
    for q in range(4):
        chance = y[:, q * 128 : q * 128 + 128]
        high, low = halves(chance * chance)
        total = lax.dot_general(
            jnp.concatenate([pick, pick], axis=1),
            jnp.concatenate([high, low], axis=1),
            (((1,), (1,)), ((), ())),
            preferred_element_type=jnp.float32,
        )
        for t in range(4):
            part = total[:, t // 2 * 128 : t // 2 * 128 + 128]
            moved = pltpu.roll(part, 64, 1)
            first, second = (moved, part) if t % 2 else (part, moved)
            marginal[t, q : q + 1, :] = jnp.where(upper, second[1:2], first[0:1])
    copies.append(pltpu.make_async_copy(marginal, marginal_out, sems.at[4]))
    copies[4].start()
    for copy in copies:
        copy.wait()


HERE, AWAY = pl.BlockSpec(memory_space=pltpu.VMEM), pl.BlockSpec(memory_space=pl.ANY)


def inner(*shape):
    return pltpu.VMEM(shape, jnp.float32)


def kept(value):
    return pltpu.with_memory_space_constraint(value, pltpu.VMEM)


def exchange(values, *chunk):
    moved = lax.all_to_all(values.reshape(256, *chunk), GROUP, 0, 0, tiled=True)
    return kept(moved.reshape(values.shape))


def on_device(amplitudes, energies, phase_angles, mix_angles):
    sent, turns = pl.pallas_call(
        first_kernel,
        out_shape=[inner(1536, 128), inner(16, 128)],
        in_specs=[AWAY] * 4,
        out_specs=[HERE, HERE],
        scratch_shapes=[
            inner(2, 4, 128, 128),
            inner(4, 128, 128),
            inner(2, 128),
            pltpu.SMEM((2, 4), jnp.float32),
            pltpu.SemaphoreType.DMA((4,)),
        ],
    )(amplitudes, energies, phase_angles, mix_angles)
    turns = kept(turns)
    arrived = exchange(sent, 3, 2, 128)
    sent = pl.pallas_call(
        second_kernel, out_shape=inner(2048, 128), in_specs=[HERE, HERE], out_specs=HERE
    )(arrived, turns)
    arrived = exchange(sent, 8, 128)
    return pl.pallas_call(
        third_kernel,
        out_shape=[
            jax.ShapeDtypeStruct((2, 4, 128, 128), jnp.float32),
            jax.ShapeDtypeStruct((4, 4, 128), jnp.float32),
        ],
        in_specs=[HERE, HERE],
        out_specs=[AWAY, AWAY],
        scratch_shapes=[inner(2, 4, 128, 128), inner(4, 4, 128), pltpu.SemaphoreType.DMA((5,))],
    )(arrived, turns)


def solution(mesh):
    parted = Mesh(mesh.devices.reshape(2, 4, 4, 4, 2), AXES)
    return jax.shard_map(
        on_device,
        mesh=parted,
        in_specs=(P(None, AXES, None, None), P(AXES, None, None), P(), P()),
        out_specs=(P(None, AXES, None, None), P(AXES[3:], AXES[:3], None)),
        check_vma=False,
    )
```

```python
import jax
import jax.numpy as jnp
from jax import lax
from jax.experimental import pallas as pl
from jax.experimental.pallas import tpu as pltpu
from jax.sharding import Mesh, PartitionSpec as P


ROT, ROT_T, FLIP = 0, 1, 2
AXES = ("zh", "y", "x", "zl", "core")
GROUP = ("zh", "zl", "y", "x", "core")


def trig(h):
    y = h * h
    c = jnp.full_like(h, -1.0 / 3628800.0)
    s = jnp.full_like(h, -1.0 / 39916800.0)
    for k in (40320.0, -720.0, 24.0, -2.0):
        c = c * y + 1.0 / k
    for k in (362880.0, -5040.0, 120.0, -6.0, 1.0):
        s = s * y + 1.0 / k
    s = s * h
    twice = s + s
    return 1.0 - twice * s, twice + twice * (c * y)


def angle(turns, layer, group):
    k = layer * 4 + group
    return turns[k : k + 1, :], turns[8 + k : 9 + k, :]


def iota(shape, dim):
    return lax.broadcasted_iota(jnp.int32, shape, dim)


def bit(value, k):
    return (value >> k) & 1


def pop(value, bits):
    total = bit(value, 0)
    for k in range(1, bits):
        total = total + bit(value, k)
    return total


def pair(kind, c, s):
    if kind == ROT:
        return c, s, -s, c
    if kind == ROT_T:
        return c, -s, s, c
    return c, s, s, -c


def table(pairs, width=128):
    j = iota((1, width), 1)
    i = iota((8, 1), 0)
    out = jnp.ones((8, width), jnp.float32)
    for k, kj, kind, c, s in pairs:
        if width > 128:
            c, s = jnp.concatenate([c, c], axis=1), jnp.concatenate([s, s], axis=1)
        a00, a01, a10, a11 = pair(kind, c, s)
        odd = bit(j, kj) == 1
        upper, lower = jnp.where(odd, a01, a00), jnp.where(odd, a11, a10)
        if k < 3:
            out = out * jnp.where(bit(i, k) == 1, lower, upper)
        else:
            out = jnp.concatenate([out * upper, out * lower], axis=0)
    return out


def doubled(small, kind, c, s):
    a00, a01, a10, a11 = pair(kind, c, s)
    top = jnp.concatenate([small * a00, small * a01], axis=1)
    low = jnp.concatenate([small * a10, small * a11], axis=1)
    return jnp.concatenate([top, low], axis=0)


def halves(x):
    high = x.astype(jnp.bfloat16)
    return high, (x - high.astype(jnp.float32)).astype(jnp.bfloat16)


def mm(a, b):
    bh, bl = halves(b)
    b = jnp.concatenate([bh, bl, bh], axis=0)
    out = []
    for part in jnp.split(a, 2, axis=0):
        ah, al = halves(part)
        out.append(jnp.dot(jnp.concatenate([ah, ah, al], axis=1), b, preferred_element_type=jnp.float32))
    return jnp.concatenate(out, axis=0)


def own_pop():
    return sum(pop(lax.axis_index(axis), 1 if axis in ("zh", "core") else 2) for axis in AXES)


def quarter_turns(extra):
    p = pop(iota((8, 128), 0), 3) + pop(iota((8, 128), 1), 7) + extra
    kinds = [(bit(p + k, 0), 1.0 - 2.0 * bit(p + k, 1).astype(jnp.float32)) for k in range(4)]
    kinds = [kinds[bin(v).count("1") % 4] for v in range(16)]
    return [jnp.concatenate(part, axis=0) for part in zip(*kinds)]


def first_kernel(amp_in, en_in, ph_in, mix_in, out, turns, amp, en, ph, mix, sems):
    copies = [(mix_in, mix), (ph_in, ph), (en_in, en), (amp_in, amp)]
    copies = [pltpu.make_async_copy(a, b, sems.at[k]) for k, (a, b) in enumerate(copies)]
    for copy in copies:
        copy.start()
    own = own_pop()
    quarters = [quarter_turns(own + k) for k in range(3)]
    for copy in copies:
        copy.wait()
    half = ph[...] * 0.5
    xr, xi = [], []
    for t in range(4):
        odd, sign = quarters[bin(t).count("1")]
        odd = odd == 1
        e = en[t]
        c, s = trig(half[0:1] * e)
        c, s = jnp.where(odd, -s, c) * sign, jnp.where(odd, c, s) * sign
        re, im = amp[0, t], amp[1, t]
        xr.append(re * c + im * s)
        xi.append(im * c - re * s)
        e2 = (half[1:2] * e).T
        for lb in range(2):
            out[pl.ds(t * 64 * 6 + 4 + lb, 64, stride=6), :] = e2[lb * 64 : lb * 64 + 64]
    row = iota((8, 128), 0)
    b = jnp.zeros((8, 128), jnp.float32)
    for k in range(8):
        b = jnp.where(row == k, mix[k // 4, k % 4], b)
    c, s = trig(b * 0.5)
    turns[0:8, :] = c
    turns[8:16, :] = s
    bits = range(7)
    c2, s2 = angle(turns, 0, 2)
    c, s = angle(turns, 0, 0)
    lanes = doubled(table([(k, k, ROT_T, c, s) for k in bits]), ROT_T, c2, s2)
    c, s = angle(turns, 0, 1)
    rows = doubled(table([(k, k, ROT_T, c, s) for k in bits]), ROT_T, c2, s2)
    x = [jnp.concatenate([v[t], v[t + 1]], axis=1) for v in (xr, xi) for t in (0, 2)]
    y = mm(jnp.concatenate(x, axis=0), lanes)
    z = []
    for c in range(2):
        for low in range(2):
            part = [
                y[(c * 2 + high) * 128 : (c * 2 + high) * 128 + 128, low * 128 : low * 128 + 128].T
                for high in range(2)
            ]
            z.append(jnp.concatenate(part, axis=1))
    y = mm(jnp.concatenate(z, axis=0), rows)
    for c in range(2):
        for t in range(4):
            for lb in range(2):
                at = (c * 2 + t % 2) * 128 + lb * 64
                out[pl.ds(t * 64 * 6 + c * 2 + lb, 64, stride=6), :] = y[at : at + 64, t // 2 * 128 : t // 2 * 128 + 128]


MIDDLE = (0, 5, 6)
SORTED = (1, 2, 3, 4, 7, 0, 5, 6)


def device_bits(turns, layer, kind, order):
    return table([(k, kj, kind, *angle(turns, layer, 3 if kj in MIDDLE else 2)) for k, kj in enumerate(order)], 256)


def second_kernel(arrived, turns, out):
    x = jnp.concatenate([arrived[pl.ds(k, 256, stride=6), :] for k in range(4)], axis=1)
    y = mm(device_bits(turns, 0, ROT, range(8)), x)
    z = [None] * 4
    for lb in range(2):
        c, s = trig(arrived[pl.ds(4 + lb, 256, stride=6), :])
        re, im = y[:, lb * 128 : lb * 128 + 128], y[:, 256 + lb * 128 : 384 + lb * 128]
        z[lb] = re * c + im * s
        z[2 + lb] = im * c - re * s
    c1, s1 = angle(turns, 1, 1)
    moved = (5, 6, 0, 1, 2, 3, 4)
    rows = table([(k, moved[k], FLIP, c1, s1) for k in range(7)])
    c0, s0 = angle(turns, 1, 0)
    z = jnp.concatenate(
        [jnp.concatenate(z[:2], axis=1), jnp.concatenate(z[2:], axis=1)], axis=0
    )
    z = mm(z, doubled(rows, FLIP, c0, s0))
    v = mm(device_bits(turns, 1, FLIP, SORTED), jnp.concatenate([z[:256], z[256:]], axis=1))
    v = [v[:, k * 128 : k * 128 + 128] for k in range(4)]
    for m in range(8):
        to = [(zh * 128 + (m // 2) * 32 + m % 2) * 8 for zh in range(2)]
        for k in range(4):
            for zh in range(2):
                at = m * 32 + zh * 16
                out[pl.ds(to[zh] + k, 16, stride=16), :] = v[k][at : at + 16]
        a = jnp.concatenate([v[k][m * 32 : m * 32 + 32] for k in range(4)], axis=0).T
        for q in range(4):
            for zh in range(2):
                at = q * 32 + zh * 16
                out[pl.ds(to[zh] + 4 + q, 16, stride=16), :] = a[at : at + 16]


def third_kernel(arrived, turns, final_out, marginal_out, final, marginal, sems):
    c0, s0 = angle(turns, 1, 0)
    c2, s2 = angle(turns, 1, 2)
    small = table([(k, k, FLIP, c0, s0) for k in range(6)] + [(6, 6, FLIP, c2, s2)])
    w = doubled(small, FLIP, c2, s2)
    y = mm(w, jnp.concatenate([arrived[pl.ds(k, 256, stride=8), :] for k in range(4)], axis=1))
    own = own_pop()
    quarters = [quarter_turns(own + k) for k in range(3)]
    copies = []
    for t in range(4):
        odd, sign = quarters[bin(t).count("1")]
        odd = odd == 1
        f = []
        for c in range(2):
            part = [y[t * 64 : t * 64 + 64, (c * 2 + lb) * 128 : (c * 2 + lb) * 128 + 128] for lb in range(2)]
            f.append(jnp.concatenate(part, axis=0).T)
        re, im = jnp.where(odd, f[1], f[0]) * sign, jnp.where(odd, -f[0], f[1]) * sign
        for q in range(4):
            final[0, t, pl.ds(q, 32, stride=4), :] = re[q * 32 : q * 32 + 32]
            final[1, t, pl.ds(q, 32, stride=4), :] = im[q * 32 : q * 32 + 32]
        copies.append(pltpu.make_async_copy(final.at[:, t], final_out.at[:, t], sems.at[t]))
        copies[t].start()
    y = mm(w, jnp.concatenate([arrived[pl.ds(4 + k, 256, stride=8), :] for k in range(4)], axis=1))
    pick = jnp.where(bit(iota((8, 128), 1), 5) == iota((8, 128), 0), 1.0 / 32.0, 0.0).astype(jnp.bfloat16)
    upper = iota((1, 128), 1) >= 64
    for q in range(4):
        chance = y[:, q * 128 : q * 128 + 128]
        high, low = halves(chance * chance)
        total = lax.dot_general(
            jnp.concatenate([pick, pick], axis=1),
            jnp.concatenate([high, low], axis=1),
            (((1,), (1,)), ((), ())),
            preferred_element_type=jnp.float32,
        )
        for t in range(4):
            part = total[:, t // 2 * 128 : t // 2 * 128 + 128]
            moved = pltpu.roll(part, 64, 1)
            first, second = (moved, part) if t % 2 else (part, moved)
            marginal[t, q : q + 1, :] = jnp.where(upper, second[1:2], first[0:1])
    copies.append(pltpu.make_async_copy(marginal, marginal_out, sems.at[4]))
    copies[4].start()
    for copy in copies:
        copy.wait()


HERE, AWAY = pl.BlockSpec(memory_space=pltpu.VMEM), pl.BlockSpec(memory_space=pl.ANY)


def inner(*shape):
    return pltpu.VMEM(shape, jnp.float32)


def kept(value):
    return pltpu.with_memory_space_constraint(value, pltpu.VMEM)


def exchange(values, *chunk):
    moved = lax.all_to_all(values.reshape(256, *chunk), GROUP, 0, 0, tiled=True)
    return kept(moved.reshape(values.shape))


def on_device(amplitudes, energies, phase_angles, mix_angles):
    sent, turns = pl.pallas_call(
        first_kernel,
        out_shape=[inner(1536, 128), inner(16, 128)],
        in_specs=[AWAY] * 4,
        out_specs=[HERE, HERE],
        scratch_shapes=[
            inner(2, 4, 128, 128),
            inner(4, 128, 128),
            inner(2, 128),
            pltpu.SMEM((2, 4), jnp.float32),
            pltpu.SemaphoreType.DMA((4,)),
        ],
    )(amplitudes, energies, phase_angles, mix_angles)
    turns = kept(turns)
    arrived = exchange(sent, 3, 2, 128)
    sent = pl.pallas_call(
        second_kernel, out_shape=inner(2048, 128), in_specs=[HERE, HERE], out_specs=HERE
    )(arrived, turns)
    arrived = exchange(sent, 8, 128)
    return pl.pallas_call(
        third_kernel,
        out_shape=[
            jax.ShapeDtypeStruct((2, 4, 128, 128), jnp.float32),
            jax.ShapeDtypeStruct((4, 4, 128), jnp.float32),
        ],
        in_specs=[HERE, HERE],
        out_specs=[AWAY, AWAY],
        scratch_shapes=[inner(2, 4, 128, 128), inner(4, 4, 128), pltpu.SemaphoreType.DMA((5,))],
    )(arrived, turns)


def solution(mesh):
    parted = Mesh(mesh.devices.reshape(2, 4, 4, 4, 2), AXES)
    return jax.shard_map(
        on_device,
        mesh=parted,
        in_specs=(P(None, AXES, None, None), P(AXES, None, None), P(), P()),
        out_specs=(P(None, AXES, None, None), P(AXES[3:], AXES[:3], None)),
        check_vma=False,
    )
```

```python
import jax
import jax.numpy as jnp
from jax import lax
from jax.experimental import pallas as pl
from jax.experimental.pallas import tpu as pltpu
from jax.sharding import Mesh, PartitionSpec as P


ROT, ROT_T, FLIP = 0, 1, 2
AXES = ("zh", "y", "x", "zl", "core")
GROUP = ("zh", "zl", "y", "x", "core")


def trig(h):
    y = h * h
    c = jnp.full_like(h, -1.0 / 3628800.0)
    s = jnp.full_like(h, -1.0 / 39916800.0)
    for k in (40320.0, -720.0, 24.0, -2.0):
        c = c * y + 1.0 / k
    for k in (362880.0, -5040.0, 120.0, -6.0, 1.0):
        s = s * y + 1.0 / k
    s = s * h
    twice = s + s
    return 1.0 - twice * s, twice + twice * (c * y)


def angle(turns, layer, group):
    k = layer * 4 + group
    return turns[k : k + 1, :], turns[8 + k : 9 + k, :]


def iota(shape, dim):
    return lax.broadcasted_iota(jnp.int32, shape, dim)


def bit(value, k):
    return (value >> k) & 1


def pop(value, bits):
    total = bit(value, 0)
    for k in range(1, bits):
        total = total + bit(value, k)
    return total


def pair(kind, c, s):
    if kind == ROT:
        return c, s, -s, c
    if kind == ROT_T:
        return c, -s, s, c
    return c, s, s, -c


def table(pairs, width=128):
    j = iota((1, width), 1)
    i = iota((8, 1), 0)
    out = jnp.ones((8, width), jnp.float32)
    for k, kj, kind, c, s in pairs:
        if width > 128:
            c, s = jnp.concatenate([c, c], axis=1), jnp.concatenate([s, s], axis=1)
        a00, a01, a10, a11 = pair(kind, c, s)
        odd = bit(j, kj) == 1
        upper, lower = jnp.where(odd, a01, a00), jnp.where(odd, a11, a10)
        if k < 3:
            out = out * jnp.where(bit(i, k) == 1, lower, upper)
        else:
            out = jnp.concatenate([out * upper, out * lower], axis=0)
    return out


def doubled(small, kind, c, s):
    a00, a01, a10, a11 = pair(kind, c, s)
    top = jnp.concatenate([small * a00, small * a01], axis=1)
    low = jnp.concatenate([small * a10, small * a11], axis=1)
    return jnp.concatenate([top, low], axis=0)


def halves(x):
    high = x.astype(jnp.bfloat16)
    return high, (x - high.astype(jnp.float32)).astype(jnp.bfloat16)


def mm(a, b):
    bh, bl = halves(b)
    b = jnp.concatenate([bh, bl, bh], axis=0)
    out = []
    for part in jnp.split(a, 2, axis=0):
        ah, al = halves(part)
        out.append(jnp.dot(jnp.concatenate([ah, ah, al], axis=1), b, preferred_element_type=jnp.float32))
    return jnp.concatenate(out, axis=0)


def own_pop():
    return sum(pop(lax.axis_index(axis), 1 if axis in ("zh", "core") else 2) for axis in AXES)


def quarter_turns(extra):
    p = pop(iota((8, 128), 0), 3) + pop(iota((8, 128), 1), 7) + extra
    kinds = [(bit(p + k, 0), 1.0 - 2.0 * bit(p + k, 1).astype(jnp.float32)) for k in range(4)]
    kinds = [kinds[bin(v).count("1") % 4] for v in range(16)]
    return [jnp.concatenate(part, axis=0) for part in zip(*kinds)]


def first_kernel(amp_in, en_in, ph_in, mix_in, out, turns, amp, en, ph, mix, sems):
    copies = [(mix_in, mix), (ph_in, ph), (en_in, en), (amp_in, amp)]
    copies = [pltpu.make_async_copy(a, b, sems.at[k]) for k, (a, b) in enumerate(copies)]
    for copy in copies:
        copy.start()
    own = own_pop()
    quarters = [quarter_turns(own + k) for k in range(3)]
    copies[0].wait()
    row = iota((8, 128), 0)
    b = jnp.zeros((8, 128), jnp.float32)
    for k in range(8):
        b = jnp.where(row == k, mix[k // 4, k % 4], b)
    c, s = trig(b * 0.5)
    turns[0:8, :] = c
    turns[8:16, :] = s
    bits = range(7)
    c2, s2 = angle(turns, 0, 2)
    c, s = angle(turns, 0, 0)
    lanes = doubled(table([(k, k, ROT_T, c, s) for k in bits]), ROT_T, c2, s2)
    c, s = angle(turns, 0, 1)
    rows = doubled(table([(k, k, ROT_T, c, s) for k in bits]), ROT_T, c2, s2)
    for copy in copies[1:]:
        copy.wait()
    half = ph[...] * 0.5
    xr, xi = [], []
    for t in range(4):
        odd, sign = quarters[bin(t).count("1")]
        odd = odd == 1
        e = en[t]
        c, s = trig(half[0:1] * e)
        c, s = jnp.where(odd, -s, c) * sign, jnp.where(odd, c, s) * sign
        re, im = amp[0, t], amp[1, t]
        xr.append(re * c + im * s)
        xi.append(im * c - re * s)
        e2 = (half[1:2] * e).T
        for lb in range(2):
            out[pl.ds(t * 64 * 6 + 4 + lb, 64, stride=6), :] = e2[lb * 64 : lb * 64 + 64]
    x = [jnp.concatenate([v[t], v[t + 1]], axis=1) for v in (xr, xi) for t in (0, 2)]
    y = mm(jnp.concatenate(x, axis=0), lanes)
    z = []
    for c in range(2):
        for low in range(2):
            part = [
                y[(c * 2 + high) * 128 : (c * 2 + high) * 128 + 128, low * 128 : low * 128 + 128].T
                for high in range(2)
            ]
            z.append(jnp.concatenate(part, axis=1))
    y = mm(jnp.concatenate(z, axis=0), rows)
    for c in range(2):
        for t in range(4):
            for lb in range(2):
                at = (c * 2 + t % 2) * 128 + lb * 64
                out[pl.ds(t * 64 * 6 + c * 2 + lb, 64, stride=6), :] = y[at : at + 64, t // 2 * 128 : t // 2 * 128 + 128]


MIDDLE = (0, 5, 6)
SORTED = (1, 2, 3, 4, 7, 0, 5, 6)


def device_bits(turns, layer, kind, order):
    return table([(k, kj, kind, *angle(turns, layer, 3 if kj in MIDDLE else 2)) for k, kj in enumerate(order)], 256)


def second_kernel(arrived, turns, out):
    x = jnp.concatenate([arrived[pl.ds(k, 256, stride=6), :] for k in range(4)], axis=1)
    y = mm(device_bits(turns, 0, ROT, range(8)), x)
    z = [None] * 4
    for lb in range(2):
        c, s = trig(arrived[pl.ds(4 + lb, 256, stride=6), :])
        re, im = y[:, lb * 128 : lb * 128 + 128], y[:, 256 + lb * 128 : 384 + lb * 128]
        z[lb] = re * c + im * s
        z[2 + lb] = im * c - re * s
    c1, s1 = angle(turns, 1, 1)
    moved = (5, 6, 0, 1, 2, 3, 4)
    rows = table([(k, moved[k], FLIP, c1, s1) for k in range(7)])
    c0, s0 = angle(turns, 1, 0)
    z = jnp.concatenate(
        [jnp.concatenate(z[:2], axis=1), jnp.concatenate(z[2:], axis=1)], axis=0
    )
    z = mm(z, doubled(rows, FLIP, c0, s0))
    v = mm(device_bits(turns, 1, FLIP, SORTED), jnp.concatenate([z[:256], z[256:]], axis=1))
    v = [v[:, k * 128 : k * 128 + 128] for k in range(4)]
    for m in range(8):
        to = [(zh * 128 + (m // 2) * 32 + m % 2) * 8 for zh in range(2)]
        for k in range(4):
            for zh in range(2):
                at = m * 32 + zh * 16
                out[pl.ds(to[zh] + k, 16, stride=16), :] = v[k][at : at + 16]
        a = jnp.concatenate([v[k][m * 32 : m * 32 + 32] for k in range(4)], axis=0).T
        for q in range(4):
            for zh in range(2):
                at = q * 32 + zh * 16
                out[pl.ds(to[zh] + 4 + q, 16, stride=16), :] = a[at : at + 16]


def third_kernel(arrived, turns, final_out, marginal_out, final, marginal, sems):
    c0, s0 = angle(turns, 1, 0)
    c2, s2 = angle(turns, 1, 2)
    small = table([(k, k, FLIP, c0, s0) for k in range(6)] + [(6, 6, FLIP, c2, s2)])
    w = doubled(small, FLIP, c2, s2)
    y = mm(w, jnp.concatenate([arrived[pl.ds(k, 256, stride=8), :] for k in range(4)], axis=1))
    own = own_pop()
    quarters = [quarter_turns(own + k) for k in range(3)]
    copies = []
    for t in range(4):
        odd, sign = quarters[bin(t).count("1")]
        odd = odd == 1
        f = []
        for c in range(2):
            part = [y[t * 64 : t * 64 + 64, (c * 2 + lb) * 128 : (c * 2 + lb) * 128 + 128] for lb in range(2)]
            f.append(jnp.concatenate(part, axis=0).T)
        re, im = jnp.where(odd, f[1], f[0]) * sign, jnp.where(odd, -f[0], f[1]) * sign
        for q in range(4):
            final[0, t, pl.ds(q, 32, stride=4), :] = re[q * 32 : q * 32 + 32]
            final[1, t, pl.ds(q, 32, stride=4), :] = im[q * 32 : q * 32 + 32]
        copies.append(pltpu.make_async_copy(final.at[:, t], final_out.at[:, t], sems.at[t]))
        copies[t].start()
    y = mm(w, jnp.concatenate([arrived[pl.ds(4 + k, 256, stride=8), :] for k in range(4)], axis=1))
    pick = jnp.where(bit(iota((8, 128), 1), 5) == iota((8, 128), 0), 1.0 / 32.0, 0.0).astype(jnp.bfloat16)
    upper = iota((1, 128), 1) >= 64
    for q in range(4):
        chance = y[:, q * 128 : q * 128 + 128]
        high, low = halves(chance * chance)
        total = lax.dot_general(
            jnp.concatenate([pick, pick], axis=1),
            jnp.concatenate([high, low], axis=1),
            (((1,), (1,)), ((), ())),
            preferred_element_type=jnp.float32,
        )
        for t in range(4):
            part = total[:, t // 2 * 128 : t // 2 * 128 + 128]
            moved = pltpu.roll(part, 64, 1)
            first, second = (moved, part) if t % 2 else (part, moved)
            marginal[t, q : q + 1, :] = jnp.where(upper, second[1:2], first[0:1])
    copies.append(pltpu.make_async_copy(marginal, marginal_out, sems.at[4]))
    copies[4].start()
    for copy in copies:
        copy.wait()


HERE, AWAY = pl.BlockSpec(memory_space=pltpu.VMEM), pl.BlockSpec(memory_space=pl.ANY)


def inner(*shape):
    return pltpu.VMEM(shape, jnp.float32)


def kept(value):
    return pltpu.with_memory_space_constraint(value, pltpu.VMEM)


def exchange(values, *chunk):
    moved = lax.all_to_all(values.reshape(256, *chunk), GROUP, 0, 0, tiled=True)
    return kept(moved.reshape(values.shape))


def on_device(amplitudes, energies, phase_angles, mix_angles):
    sent, turns = pl.pallas_call(
        first_kernel,
        out_shape=[inner(1536, 128), inner(16, 128)],
        in_specs=[AWAY] * 4,
        out_specs=[HERE, HERE],
        scratch_shapes=[
            inner(2, 4, 128, 128),
            inner(4, 128, 128),
            inner(2, 128),
            pltpu.SMEM((2, 4), jnp.float32),
            pltpu.SemaphoreType.DMA((4,)),
        ],
    )(amplitudes, energies, phase_angles, mix_angles)
    turns = kept(turns)
    arrived = exchange(sent, 3, 2, 128)
    sent = pl.pallas_call(
        second_kernel, out_shape=inner(2048, 128), in_specs=[HERE, HERE], out_specs=HERE
    )(arrived, turns)
    arrived = exchange(sent, 8, 128)
    return pl.pallas_call(
        third_kernel,
        out_shape=[
            jax.ShapeDtypeStruct((2, 4, 128, 128), jnp.float32),
            jax.ShapeDtypeStruct((4, 4, 128), jnp.float32),
        ],
        in_specs=[HERE, HERE],
        out_specs=[AWAY, AWAY],
        scratch_shapes=[inner(2, 4, 128, 128), inner(4, 4, 128), pltpu.SemaphoreType.DMA((5,))],
    )(arrived, turns)


def solution(mesh):
    parted = Mesh(mesh.devices.reshape(2, 4, 4, 4, 2), AXES)
    return jax.shard_map(
        on_device,
        mesh=parted,
        in_specs=(P(None, AXES, None, None), P(AXES, None, None), P(), P()),
        out_specs=(P(None, AXES, None, None), P(AXES[3:], AXES[:3], None)),
        check_vma=False,
    )
```

```python
import jax
import jax.numpy as jnp
from jax import lax
from jax.experimental import pallas as pl
from jax.experimental.pallas import tpu as pltpu
from jax.sharding import Mesh, PartitionSpec as P


ROT, ROT_T, FLIP = 0, 1, 2
AXES = ("zh", "y", "x", "zl", "core")
GROUP = ("zh", "zl", "y", "x", "core")


def trig(h):
    y = h * h
    c = jnp.full_like(h, -1.0 / 3628800.0)
    s = jnp.full_like(h, -1.0 / 39916800.0)
    for k in (40320.0, -720.0, 24.0, -2.0):
        c = c * y + 1.0 / k
    for k in (362880.0, -5040.0, 120.0, -6.0, 1.0):
        s = s * y + 1.0 / k
    s = s * h
    twice = s + s
    return 1.0 - twice * s, twice + twice * (c * y)


def angle(turns, layer, group):
    k = layer * 4 + group
    return turns[k : k + 1, :], turns[8 + k : 9 + k, :]


def iota(shape, dim):
    return lax.broadcasted_iota(jnp.int32, shape, dim)


def bit(value, k):
    return (value >> k) & 1


def pop(value, bits):
    total = bit(value, 0)
    for k in range(1, bits):
        total = total + bit(value, k)
    return total


def pair(kind, c, s):
    if kind == ROT:
        return c, s, -s, c
    if kind == ROT_T:
        return c, -s, s, c
    return c, s, s, -c


def table(pairs, width=128):
    j = iota((1, width), 1)
    i = iota((8, 1), 0)
    out = jnp.ones((8, width), jnp.float32)
    for k, kj, kind, c, s in pairs:
        if width > 128:
            c, s = jnp.concatenate([c, c], axis=1), jnp.concatenate([s, s], axis=1)
        a00, a01, a10, a11 = pair(kind, c, s)
        odd = bit(j, kj) == 1
        upper, lower = jnp.where(odd, a01, a00), jnp.where(odd, a11, a10)
        if k < 3:
            out = out * jnp.where(bit(i, k) == 1, lower, upper)
        else:
            out = jnp.concatenate([out * upper, out * lower], axis=0)
    return out


def doubled(small, kind, c, s):
    a00, a01, a10, a11 = pair(kind, c, s)
    top = jnp.concatenate([small * a00, small * a01], axis=1)
    low = jnp.concatenate([small * a10, small * a11], axis=1)
    return jnp.concatenate([top, low], axis=0)


def halves(x):
    high = x.astype(jnp.bfloat16)
    return high, (x - high.astype(jnp.float32)).astype(jnp.bfloat16)


def mm(a, b):
    bh, bl = halves(b)
    b = jnp.concatenate([bh, bl, bh], axis=0)
    out = []
    for part in jnp.split(a, 4 if a.shape[0] > 256 else 2, axis=0):
        ah, al = halves(part)
        out.append(jnp.dot(jnp.concatenate([ah, ah, al], axis=1), b, preferred_element_type=jnp.float32))
    return jnp.concatenate(out, axis=0)


def own_pop():
    return sum(pop(lax.axis_index(axis), 1 if axis in ("zh", "core") else 2) for axis in AXES)


def quarter_turns(extra):
    p = pop(iota((8, 128), 0), 3) + pop(iota((8, 128), 1), 7) + extra
    kinds = [(bit(p + k, 0), 1.0 - 2.0 * bit(p + k, 1).astype(jnp.float32)) for k in range(4)]
    kinds = [kinds[bin(v).count("1") % 4] for v in range(16)]
    return [jnp.concatenate(part, axis=0) for part in zip(*kinds)]


def first_kernel(amp_in, en_in, ph_in, mix_in, out, turns, amp, en, ph, mix, sems):
    copies = [(mix_in, mix), (ph_in, ph), (en_in, en), (amp_in, amp)]
    copies = [pltpu.make_async_copy(a, b, sems.at[k]) for k, (a, b) in enumerate(copies)]
    for copy in copies:
        copy.start()
    own = own_pop()
    quarters = [quarter_turns(own + k) for k in range(3)]
    copies[0].wait()
    row = iota((8, 128), 0)
    b = jnp.zeros((8, 128), jnp.float32)
    for k in range(8):
        b = jnp.where(row == k, mix[k // 4, k % 4], b)
    c, s = trig(b * 0.5)
    turns[0:8, :] = c
    turns[8:16, :] = s
    bits = range(7)
    c2, s2 = angle(turns, 0, 2)
    c, s = angle(turns, 0, 0)
    lanes = doubled(table([(k, k, ROT_T, c, s) for k in bits]), ROT_T, c2, s2)
    c, s = angle(turns, 0, 1)
    rows = doubled(table([(k, k, ROT_T, c, s) for k in bits]), ROT_T, c2, s2)
    for copy in copies[1:]:
        copy.wait()
    half = ph[...] * 0.5
    xr, xi = [], []
    for t in range(4):
        odd, sign = quarters[bin(t).count("1")]
        odd = odd == 1
        e = en[t]
        c, s = trig(half[0:1] * e)
        c, s = jnp.where(odd, -s, c) * sign, jnp.where(odd, c, s) * sign
        re, im = amp[0, t], amp[1, t]
        xr.append(re * c + im * s)
        xi.append(im * c - re * s)
        e2 = (half[1:2] * e).T
        for lb in range(2):
            out[pl.ds(t * 64 * 6 + 4 + lb, 64, stride=6), :] = e2[lb * 64 : lb * 64 + 64]
    x = [jnp.concatenate([v[t], v[t + 1]], axis=1) for v in (xr, xi) for t in (0, 2)]
    y = mm(jnp.concatenate(x, axis=0), lanes)
    z = []
    for c in range(2):
        for low in range(2):
            part = [
                y[(c * 2 + high) * 128 : (c * 2 + high) * 128 + 128, low * 128 : low * 128 + 128].T
                for high in range(2)
            ]
            z.append(jnp.concatenate(part, axis=1))
    y = mm(jnp.concatenate(z, axis=0), rows)
    for c in range(2):
        for t in range(4):
            for lb in range(2):
                at = (c * 2 + t % 2) * 128 + lb * 64
                out[pl.ds(t * 64 * 6 + c * 2 + lb, 64, stride=6), :] = y[at : at + 64, t // 2 * 128 : t // 2 * 128 + 128]


MIDDLE = (0, 5, 6)
SORTED = (1, 2, 3, 4, 7, 0, 5, 6)


def device_bits(turns, layer, kind, order):
    return table([(k, kj, kind, *angle(turns, layer, 3 if kj in MIDDLE else 2)) for k, kj in enumerate(order)], 256)


def second_kernel(arrived, turns, out):
    x = jnp.concatenate([arrived[pl.ds(k, 256, stride=6), :] for k in range(4)], axis=1)
    y = mm(device_bits(turns, 0, ROT, range(8)), x)
    z = [None] * 4
    for lb in range(2):
        c, s = trig(arrived[pl.ds(4 + lb, 256, stride=6), :])
        re, im = y[:, lb * 128 : lb * 128 + 128], y[:, 256 + lb * 128 : 384 + lb * 128]
        z[lb] = re * c + im * s
        z[2 + lb] = im * c - re * s
    c1, s1 = angle(turns, 1, 1)
    moved = (5, 6, 0, 1, 2, 3, 4)
    rows = table([(k, moved[k], FLIP, c1, s1) for k in range(7)])
    c0, s0 = angle(turns, 1, 0)
    z = jnp.concatenate(
        [jnp.concatenate(z[:2], axis=1), jnp.concatenate(z[2:], axis=1)], axis=0
    )
    z = mm(z, doubled(rows, FLIP, c0, s0))
    v = mm(device_bits(turns, 1, FLIP, SORTED), jnp.concatenate([z[:256], z[256:]], axis=1))
    v = [v[:, k * 128 : k * 128 + 128] for k in range(4)]
    for m in range(8):
        to = [(zh * 128 + (m // 2) * 32 + m % 2) * 8 for zh in range(2)]
        for k in range(4):
            for zh in range(2):
                at = m * 32 + zh * 16
                out[pl.ds(to[zh] + k, 16, stride=16), :] = v[k][at : at + 16]
        a = jnp.concatenate([v[k][m * 32 : m * 32 + 32] for k in range(4)], axis=0).T
        for q in range(4):
            for zh in range(2):
                at = q * 32 + zh * 16
                out[pl.ds(to[zh] + 4 + q, 16, stride=16), :] = a[at : at + 16]


def third_kernel(arrived, turns, final_out, marginal_out, final, marginal, sems):
    c0, s0 = angle(turns, 1, 0)
    c2, s2 = angle(turns, 1, 2)
    small = table([(k, k, FLIP, c0, s0) for k in range(6)] + [(6, 6, FLIP, c2, s2)])
    w = doubled(small, FLIP, c2, s2)
    y = mm(w, jnp.concatenate([arrived[pl.ds(k, 256, stride=8), :] for k in range(4)], axis=1))
    own = own_pop()
    quarters = [quarter_turns(own + k) for k in range(3)]
    copies = []
    for t in range(4):
        odd, sign = quarters[bin(t).count("1")]
        odd = odd == 1
        f = []
        for c in range(2):
            part = [y[t * 64 : t * 64 + 64, (c * 2 + lb) * 128 : (c * 2 + lb) * 128 + 128] for lb in range(2)]
            f.append(jnp.concatenate(part, axis=0).T)
        re, im = jnp.where(odd, f[1], f[0]) * sign, jnp.where(odd, -f[0], f[1]) * sign
        for q in range(4):
            final[0, t, pl.ds(q, 32, stride=4), :] = re[q * 32 : q * 32 + 32]
            final[1, t, pl.ds(q, 32, stride=4), :] = im[q * 32 : q * 32 + 32]
        copies.append(pltpu.make_async_copy(final.at[:, t], final_out.at[:, t], sems.at[t]))
        copies[t].start()
    y = mm(w, jnp.concatenate([arrived[pl.ds(4 + k, 256, stride=8), :] for k in range(4)], axis=1))
    pick = jnp.where(bit(iota((8, 128), 1), 5) == iota((8, 128), 0), 1.0 / 32.0, 0.0).astype(jnp.bfloat16)
    upper = iota((1, 128), 1) >= 64
    for q in range(4):
        chance = y[:, q * 128 : q * 128 + 128]
        high, low = halves(chance * chance)
        total = lax.dot_general(
            jnp.concatenate([pick, pick], axis=1),
            jnp.concatenate([high, low], axis=1),
            (((1,), (1,)), ((), ())),
            preferred_element_type=jnp.float32,
        )
        for t in range(4):
            part = total[:, t // 2 * 128 : t // 2 * 128 + 128]
            moved = pltpu.roll(part, 64, 1)
            first, second = (moved, part) if t % 2 else (part, moved)
            marginal[t, q : q + 1, :] = jnp.where(upper, second[1:2], first[0:1])
    copies.append(pltpu.make_async_copy(marginal, marginal_out, sems.at[4]))
    copies[4].start()
    for copy in copies:
        copy.wait()


HERE, AWAY = pl.BlockSpec(memory_space=pltpu.VMEM), pl.BlockSpec(memory_space=pl.ANY)


def inner(*shape):
    return pltpu.VMEM(shape, jnp.float32)


def kept(value):
    return pltpu.with_memory_space_constraint(value, pltpu.VMEM)


def exchange(values, *chunk):
    moved = lax.all_to_all(values.reshape(256, *chunk), GROUP, 0, 0, tiled=True)
    return kept(moved.reshape(values.shape))


def on_device(amplitudes, energies, phase_angles, mix_angles):
    sent, turns = pl.pallas_call(
        first_kernel,
        out_shape=[inner(1536, 128), inner(16, 128)],
        in_specs=[AWAY] * 4,
        out_specs=[HERE, HERE],
        scratch_shapes=[
            inner(2, 4, 128, 128),
            inner(4, 128, 128),
            inner(2, 128),
            pltpu.SMEM((2, 4), jnp.float32),
            pltpu.SemaphoreType.DMA((4,)),
        ],
    )(amplitudes, energies, phase_angles, mix_angles)
    turns = kept(turns)
    arrived = exchange(sent, 3, 2, 128)
    sent = pl.pallas_call(
        second_kernel, out_shape=inner(2048, 128), in_specs=[HERE, HERE], out_specs=HERE
    )(arrived, turns)
    arrived = exchange(sent, 8, 128)
    return pl.pallas_call(
        third_kernel,
        out_shape=[
            jax.ShapeDtypeStruct((2, 4, 128, 128), jnp.float32),
            jax.ShapeDtypeStruct((4, 4, 128), jnp.float32),
        ],
        in_specs=[HERE, HERE],
        out_specs=[AWAY, AWAY],
        scratch_shapes=[inner(2, 4, 128, 128), inner(4, 4, 128), pltpu.SemaphoreType.DMA((5,))],
    )(arrived, turns)


def solution(mesh):
    parted = Mesh(mesh.devices.reshape(2, 4, 4, 4, 2), AXES)
    return jax.shard_map(
        on_device,
        mesh=parted,
        in_specs=(P(None, AXES, None, None), P(AXES, None, None), P(), P()),
        out_specs=(P(None, AXES, None, None), P(AXES[3:], AXES[:3], None)),
        check_vma=False,
    )
```

```python
import jax
import jax.numpy as jnp
from jax import lax
from jax.experimental import pallas as pl
from jax.experimental.pallas import tpu as pltpu
from jax.sharding import Mesh, PartitionSpec as P


ROT, ROT_T, FLIP = 0, 1, 2
AXES = ("zh", "y", "x", "zl", "core")
GROUP = ("zh", "zl", "y", "x", "core")


def trig(h):
    y = h * h
    c = jnp.full_like(h, -1.0 / 3628800.0)
    s = jnp.full_like(h, -1.0 / 39916800.0)
    for k in (40320.0, -720.0, 24.0, -2.0):
        c = c * y + 1.0 / k
    for k in (362880.0, -5040.0, 120.0, -6.0, 1.0):
        s = s * y + 1.0 / k
    s = s * h
    twice = s + s
    return 1.0 - twice * s, twice + twice * (c * y)


def angle(turns, layer, group):
    k = layer * 4 + group
    return turns[k : k + 1, :], turns[8 + k : 9 + k, :]


def iota(shape, dim):
    return lax.broadcasted_iota(jnp.int32, shape, dim)


def bit(value, k):
    return (value >> k) & 1


def pop(value, bits):
    total = bit(value, 0)
    for k in range(1, bits):
        total = total + bit(value, k)
    return total


def pair(kind, c, s):
    if kind == ROT:
        return c, s, -s, c
    if kind == ROT_T:
        return c, -s, s, c
    return c, s, s, -c


def table(pairs, width=128):
    j = iota((1, width), 1)
    i = iota((8, 1), 0)
    out = jnp.ones((8, width), jnp.float32)
    for k, kj, kind, c, s in pairs:
        if width > 128:
            c, s = jnp.concatenate([c, c], axis=1), jnp.concatenate([s, s], axis=1)
        a00, a01, a10, a11 = pair(kind, c, s)
        odd = bit(j, kj) == 1
        upper, lower = jnp.where(odd, a01, a00), jnp.where(odd, a11, a10)
        if k < 3:
            out = out * jnp.where(bit(i, k) == 1, lower, upper)
        else:
            out = jnp.concatenate([out * upper, out * lower], axis=0)
    return out


def doubled(small, kind, c, s):
    a00, a01, a10, a11 = pair(kind, c, s)
    top = jnp.concatenate([small * a00, small * a01], axis=1)
    low = jnp.concatenate([small * a10, small * a11], axis=1)
    return jnp.concatenate([top, low], axis=0)


def halves(x):
    high = x.astype(jnp.bfloat16)
    return high, (x - high.astype(jnp.float32)).astype(jnp.bfloat16)


def mm(a, b):
    bh, bl = halves(b)
    b = jnp.concatenate([bh, bl, bh], axis=0)
    out = []
    for part in jnp.split(a, 4 if a.shape[0] > 256 else 2, axis=0):
        ah, al = halves(part)
        out.append(jnp.dot(jnp.concatenate([ah, ah, al], axis=1), b, preferred_element_type=jnp.float32))
    return jnp.concatenate(out, axis=0)


def own_pop():
    return sum(pop(lax.axis_index(axis), 1 if axis in ("zh", "core") else 2) for axis in AXES)


def quarter_turns(extra):
    p = pop(iota((8, 128), 0), 3) + pop(iota((8, 128), 1), 7) + extra
    kinds = [(bit(p + k, 0), 1.0 - 2.0 * bit(p + k, 1).astype(jnp.float32)) for k in range(4)]
    kinds = [kinds[bin(v).count("1") % 4] for v in range(16)]
    return [jnp.concatenate(part, axis=0) for part in zip(*kinds)]


def first_kernel(amp_in, en_in, ph_in, mix_in, out, turns, amp, en, ph, mix, sems):
    copies = [(mix_in, mix), (ph_in, ph), (en_in, en), (amp_in, amp)]
    copies = [pltpu.make_async_copy(a, b, sems.at[k]) for k, (a, b) in enumerate(copies)]
    for copy in copies:
        copy.start()
    own = own_pop()
    quarters = [quarter_turns(own + k) for k in range(3)]
    copies[0].wait()
    row = iota((8, 128), 0)
    b = jnp.zeros((8, 128), jnp.float32)
    for k in range(8):
        b = jnp.where(row == k, mix[k // 4, k % 4], b)
    c, s = trig(b * 0.5)
    turns[0:8, :] = c
    turns[8:16, :] = s
    bits = range(7)
    c2, s2 = angle(turns, 0, 2)
    c, s = angle(turns, 0, 0)
    lanes = doubled(table([(k, k, ROT_T, c, s) for k in bits]), ROT_T, c2, s2)
    c, s = angle(turns, 0, 1)
    rows = doubled(table([(k, k, ROT_T, c, s) for k in bits]), ROT_T, c2, s2)
    for copy in copies[1:]:
        copy.wait()
    half = ph[...] * 0.5
    xr, xi = [], []
    for t in range(4):
        odd, sign = quarters[bin(t).count("1")]
        odd = odd == 1
        e = en[t]
        c, s = trig(half[0:1] * e)
        flip = jnp.where(odd, -sign, sign)
        c, s = jnp.where(odd, s, c) * flip, jnp.where(odd, c, s) * sign
        re, im = amp[0, t], amp[1, t]
        xr.append(re * c + im * s)
        xi.append(im * c - re * s)
        e2 = (half[1:2] * e).T
        for lb in range(2):
            out[pl.ds(t * 64 * 6 + 4 + lb, 64, stride=6), :] = e2[lb * 64 : lb * 64 + 64]
    x = [jnp.concatenate([v[t], v[t + 1]], axis=1) for v in (xr, xi) for t in (0, 2)]
    y = mm(jnp.concatenate(x, axis=0), lanes)
    z = []
    for c in range(2):
        for low in range(2):
            part = [
                y[(c * 2 + high) * 128 : (c * 2 + high) * 128 + 128, low * 128 : low * 128 + 128].T
                for high in range(2)
            ]
            z.append(jnp.concatenate(part, axis=1))
    y = mm(jnp.concatenate(z, axis=0), rows)
    for c in range(2):
        for t in range(4):
            for lb in range(2):
                at = (c * 2 + t % 2) * 128 + lb * 64
                out[pl.ds(t * 64 * 6 + c * 2 + lb, 64, stride=6), :] = y[at : at + 64, t // 2 * 128 : t // 2 * 128 + 128]


MIDDLE = (0, 5, 6)
SORTED = (1, 2, 3, 4, 7, 0, 5, 6)


def device_bits(turns, layer, kind, order):
    return table([(k, kj, kind, *angle(turns, layer, 3 if kj in MIDDLE else 2)) for k, kj in enumerate(order)], 256)


def second_kernel(arrived, turns, out):
    x = jnp.concatenate([arrived[pl.ds(k, 256, stride=6), :] for k in range(4)], axis=1)
    y = mm(device_bits(turns, 0, ROT, range(8)), x)
    z = [None] * 4
    for lb in range(2):
        c, s = trig(arrived[pl.ds(4 + lb, 256, stride=6), :])
        re, im = y[:, lb * 128 : lb * 128 + 128], y[:, 256 + lb * 128 : 384 + lb * 128]
        z[lb] = re * c + im * s
        z[2 + lb] = im * c - re * s
    c1, s1 = angle(turns, 1, 1)
    moved = (5, 6, 0, 1, 2, 3, 4)
    rows = table([(k, moved[k], FLIP, c1, s1) for k in range(7)])
    c0, s0 = angle(turns, 1, 0)
    z = jnp.concatenate(
        [jnp.concatenate(z[:2], axis=1), jnp.concatenate(z[2:], axis=1)], axis=0
    )
    z = mm(z, doubled(rows, FLIP, c0, s0))
    v = mm(device_bits(turns, 1, FLIP, SORTED), jnp.concatenate([z[:256], z[256:]], axis=1))
    v = [v[:, k * 128 : k * 128 + 128] for k in range(4)]
    for m in range(8):
        to = [(zh * 128 + (m // 2) * 32 + m % 2) * 8 for zh in range(2)]
        for k in range(4):
            for zh in range(2):
                at = m * 32 + zh * 16
                out[pl.ds(to[zh] + k, 16, stride=16), :] = v[k][at : at + 16]
        a = jnp.concatenate([v[k][m * 32 : m * 32 + 32] for k in range(4)], axis=0).T
        for q in range(4):
            for zh in range(2):
                at = q * 32 + zh * 16
                out[pl.ds(to[zh] + 4 + q, 16, stride=16), :] = a[at : at + 16]


def third_kernel(arrived, turns, final_out, marginal_out, final, marginal, sems):
    c0, s0 = angle(turns, 1, 0)
    c2, s2 = angle(turns, 1, 2)
    small = table([(k, k, FLIP, c0, s0) for k in range(6)] + [(6, 6, FLIP, c2, s2)])
    w = doubled(small, FLIP, c2, s2)
    y = mm(w, jnp.concatenate([arrived[pl.ds(k, 256, stride=8), :] for k in range(4)], axis=1))
    own = own_pop()
    quarters = [quarter_turns(own + k) for k in range(3)]
    copies = []
    for t in range(4):
        odd, sign = quarters[bin(t).count("1")]
        odd = odd == 1
        f = []
        for c in range(2):
            part = [y[t * 64 : t * 64 + 64, (c * 2 + lb) * 128 : (c * 2 + lb) * 128 + 128] for lb in range(2)]
            f.append(jnp.concatenate(part, axis=0).T)
        flip = jnp.where(odd, -sign, sign)
        re, im = jnp.where(odd, f[1], f[0]) * sign, jnp.where(odd, f[0], f[1]) * flip
        for q in range(4):
            final[0, t, pl.ds(q, 32, stride=4), :] = re[q * 32 : q * 32 + 32]
            final[1, t, pl.ds(q, 32, stride=4), :] = im[q * 32 : q * 32 + 32]
        copies.append(pltpu.make_async_copy(final.at[:, t], final_out.at[:, t], sems.at[t]))
        copies[t].start()
    y = mm(w, jnp.concatenate([arrived[pl.ds(4 + k, 256, stride=8), :] for k in range(4)], axis=1))
    pick = jnp.where(bit(iota((8, 128), 1), 5) == iota((8, 128), 0), 1.0 / 32.0, 0.0).astype(jnp.bfloat16)
    upper = iota((1, 128), 1) >= 64
    for q in range(4):
        chance = y[:, q * 128 : q * 128 + 128]
        high, low = halves(chance * chance)
        total = lax.dot_general(
            jnp.concatenate([pick, pick], axis=1),
            jnp.concatenate([high, low], axis=1),
            (((1,), (1,)), ((), ())),
            preferred_element_type=jnp.float32,
        )
        for t in range(4):
            part = total[:, t // 2 * 128 : t // 2 * 128 + 128]
            moved = pltpu.roll(part, 64, 1)
            first, second = (moved, part) if t % 2 else (part, moved)
            marginal[t, q : q + 1, :] = jnp.where(upper, second[1:2], first[0:1])
    copies.append(pltpu.make_async_copy(marginal, marginal_out, sems.at[4]))
    copies[4].start()
    for copy in copies:
        copy.wait()


HERE, AWAY = pl.BlockSpec(memory_space=pltpu.VMEM), pl.BlockSpec(memory_space=pl.ANY)


def inner(*shape):
    return pltpu.VMEM(shape, jnp.float32)


def kept(value):
    return pltpu.with_memory_space_constraint(value, pltpu.VMEM)


def exchange(values, *chunk):
    moved = lax.all_to_all(values.reshape(256, *chunk), GROUP, 0, 0, tiled=True)
    return kept(moved.reshape(values.shape))


def on_device(amplitudes, energies, phase_angles, mix_angles):
    sent, turns = pl.pallas_call(
        first_kernel,
        out_shape=[inner(1536, 128), inner(16, 128)],
        in_specs=[AWAY] * 4,
        out_specs=[HERE, HERE],
        scratch_shapes=[
            inner(2, 4, 128, 128),
            inner(4, 128, 128),
            inner(2, 128),
            pltpu.SMEM((2, 4), jnp.float32),
            pltpu.SemaphoreType.DMA((4,)),
        ],
    )(amplitudes, energies, phase_angles, mix_angles)
    turns = kept(turns)
    arrived = exchange(sent, 3, 2, 128)
    sent = pl.pallas_call(
        second_kernel, out_shape=inner(2048, 128), in_specs=[HERE, HERE], out_specs=HERE
    )(arrived, turns)
    arrived = exchange(sent, 8, 128)
    return pl.pallas_call(
        third_kernel,
        out_shape=[
            jax.ShapeDtypeStruct((2, 4, 128, 128), jnp.float32),
            jax.ShapeDtypeStruct((4, 4, 128), jnp.float32),
        ],
        in_specs=[HERE, HERE],
        out_specs=[AWAY, AWAY],
        scratch_shapes=[inner(2, 4, 128, 128), inner(4, 4, 128), pltpu.SemaphoreType.DMA((5,))],
    )(arrived, turns)


def solution(mesh):
    parted = Mesh(mesh.devices.reshape(2, 4, 4, 4, 2), AXES)
    return jax.shard_map(
        on_device,
        mesh=parted,
        in_specs=(P(None, AXES, None, None), P(AXES, None, None), P(), P()),
        out_specs=(P(None, AXES, None, None), P(AXES[3:], AXES[:3], None)),
        check_vma=False,
    )
```

```python
import jax
import jax.numpy as jnp
from jax import lax
from jax.experimental import pallas as pl
from jax.experimental.pallas import tpu as pltpu
from jax.sharding import Mesh, PartitionSpec as P


ROT, ROT_T, FLIP = 0, 1, 2
AXES = ("zh", "y", "x", "zl", "core")
GROUP = ("zh", "zl", "y", "x", "core")


def trig(h):
    y = h * h
    c = jnp.full_like(h, -1.0 / 3628800.0)
    s = jnp.full_like(h, -1.0 / 39916800.0)
    for k in (40320.0, -720.0, 24.0, -2.0):
        c = c * y + 1.0 / k
    for k in (362880.0, -5040.0, 120.0, -6.0, 1.0):
        s = s * y + 1.0 / k
    s = s * h
    twice = s + s
    return 1.0 - twice * s, twice + twice * (c * y)


def angle(turns, layer, group):
    k = layer * 4 + group
    return turns[k : k + 1, :], turns[8 + k : 9 + k, :]


def iota(shape, dim):
    return lax.broadcasted_iota(jnp.int32, shape, dim)


def bit(value, k):
    return (value >> k) & 1


def pop(value, bits):
    total = bit(value, 0)
    for k in range(1, bits):
        total = total + bit(value, k)
    return total


def pair(kind, c, s):
    if kind == ROT:
        return c, s, -s, c
    if kind == ROT_T:
        return c, -s, s, c
    return c, s, s, -c


def table(pairs, width=128):
    j = iota((1, width), 1)
    i = iota((8, 1), 0)
    out = jnp.ones((8, width), jnp.float32)
    for k, kj, kind, c, s in pairs:
        if width > 128:
            c, s = jnp.concatenate([c, c], axis=1), jnp.concatenate([s, s], axis=1)
        a00, a01, a10, a11 = pair(kind, c, s)
        odd = bit(j, kj) == 1
        upper, lower = jnp.where(odd, a01, a00), jnp.where(odd, a11, a10)
        if k < 3:
            out = out * jnp.where(bit(i, k) == 1, lower, upper)
        else:
            out = jnp.concatenate([out * upper, out * lower], axis=0)
    return out


def doubled(small, kind, c, s):
    a00, a01, a10, a11 = pair(kind, c, s)
    top = jnp.concatenate([small * a00, small * a01], axis=1)
    low = jnp.concatenate([small * a10, small * a11], axis=1)
    return jnp.concatenate([top, low], axis=0)


def halves(x):
    high = x.astype(jnp.bfloat16)
    return high, (x - high.astype(jnp.float32)).astype(jnp.bfloat16)


def mm(a, b):
    bh, bl = halves(b)
    b = jnp.concatenate([bh, bl, bh], axis=0)
    out = []
    for part in jnp.split(a, 4 if a.shape[0] > 256 else 2, axis=0):
        ah, al = halves(part)
        out.append(jnp.dot(jnp.concatenate([ah, ah, al], axis=1), b, preferred_element_type=jnp.float32))
    return jnp.concatenate(out, axis=0)


def own_pop():
    return sum(pop(lax.axis_index(axis), 1 if axis in ("zh", "core") else 2) for axis in AXES)


def quarter_turns(extra):
    p = pop(iota((8, 128), 0), 3) + pop(iota((8, 128), 1), 7) + extra
    kinds = [(bit(p + k, 0), 1.0 - 2.0 * bit(p + k, 1).astype(jnp.float32)) for k in range(4)]
    kinds = [kinds[bin(v).count("1") % 4] for v in range(16)]
    return [jnp.concatenate(part, axis=0) for part in zip(*kinds)]


def first_kernel(amp_in, en_in, ph_in, mix_in, out, turns, amp, en, ph, mix, sems):
    copies = [(mix_in, mix), (ph_in, ph), (en_in, en), (amp_in.at[0], amp.at[0]), (amp_in.at[1], amp.at[1])]
    copies = [pltpu.make_async_copy(a, b, sems.at[k]) for k, (a, b) in enumerate(copies)]
    for copy in copies:
        copy.start()
    own = own_pop()
    quarters = [quarter_turns(own + k) for k in range(3)]
    copies[0].wait()
    row = iota((8, 128), 0)
    b = jnp.zeros((8, 128), jnp.float32)
    for k in range(8):
        b = jnp.where(row == k, mix[k // 4, k % 4], b)
    c, s = trig(b * 0.5)
    turns[0:8, :] = c
    turns[8:16, :] = s
    bits = range(7)
    c2, s2 = angle(turns, 0, 2)
    c, s = angle(turns, 0, 0)
    lanes = doubled(table([(k, k, ROT_T, c, s) for k in bits]), ROT_T, c2, s2)
    c, s = angle(turns, 0, 1)
    rows = doubled(table([(k, k, ROT_T, c, s) for k in bits]), ROT_T, c2, s2)
    for copy in copies[1:]:
        copy.wait()
    half = ph[...] * 0.5
    xr, xi = [], []
    for t in range(4):
        odd, sign = quarters[bin(t).count("1")]
        odd = odd == 1
        e = en[t]
        c, s = trig(half[0:1] * e)
        c, s = jnp.where(odd, -s, c) * sign, jnp.where(odd, c, s) * sign
        re, im = amp[0, t], amp[1, t]
        xr.append(re * c + im * s)
        xi.append(im * c - re * s)
        e2 = (half[1:2] * e).T
        for lb in range(2):
            out[pl.ds(t * 64 * 6 + 4 + lb, 64, stride=6), :] = e2[lb * 64 : lb * 64 + 64]
    x = [jnp.concatenate([v[t], v[t + 1]], axis=1) for v in (xr, xi) for t in (0, 2)]
    y = mm(jnp.concatenate(x, axis=0), lanes)
    z = []
    for c in range(2):
        for low in range(2):
            part = [
                y[(c * 2 + high) * 128 : (c * 2 + high) * 128 + 128, low * 128 : low * 128 + 128].T
                for high in range(2)
            ]
            z.append(jnp.concatenate(part, axis=1))
    y = mm(jnp.concatenate(z, axis=0), rows)
    for c in range(2):
        for t in range(4):
            for lb in range(2):
                at = (c * 2 + t % 2) * 128 + lb * 64
                out[pl.ds(t * 64 * 6 + c * 2 + lb, 64, stride=6), :] = y[at : at + 64, t // 2 * 128 : t // 2 * 128 + 128]


MIDDLE = (0, 5, 6)
SORTED = (1, 2, 3, 4, 7, 0, 5, 6)


def device_bits(turns, layer, kind, order):
    return table([(k, kj, kind, *angle(turns, layer, 3 if kj in MIDDLE else 2)) for k, kj in enumerate(order)], 256)


def second_kernel(arrived, turns, out):
    x = jnp.concatenate([arrived[pl.ds(k, 256, stride=6), :] for k in range(4)], axis=1)
    y = mm(device_bits(turns, 0, ROT, range(8)), x)
    z = [None] * 4
    for lb in range(2):
        c, s = trig(arrived[pl.ds(4 + lb, 256, stride=6), :])
        re, im = y[:, lb * 128 : lb * 128 + 128], y[:, 256 + lb * 128 : 384 + lb * 128]
        z[lb] = re * c + im * s
        z[2 + lb] = im * c - re * s
    c1, s1 = angle(turns, 1, 1)
    moved = (5, 6, 0, 1, 2, 3, 4)
    rows = table([(k, moved[k], FLIP, c1, s1) for k in range(7)])
    c0, s0 = angle(turns, 1, 0)
    z = jnp.concatenate(
        [jnp.concatenate(z[:2], axis=1), jnp.concatenate(z[2:], axis=1)], axis=0
    )
    z = mm(z, doubled(rows, FLIP, c0, s0))
    v = mm(device_bits(turns, 1, FLIP, SORTED), jnp.concatenate([z[:256], z[256:]], axis=1))
    v = [v[:, k * 128 : k * 128 + 128] for k in range(4)]
    for m in range(8):
        to = [(zh * 128 + (m // 2) * 32 + m % 2) * 8 for zh in range(2)]
        for k in range(4):
            for zh in range(2):
                at = m * 32 + zh * 16
                out[pl.ds(to[zh] + k, 16, stride=16), :] = v[k][at : at + 16]
        a = jnp.concatenate([v[k][m * 32 : m * 32 + 32] for k in range(4)], axis=0).T
        for q in range(4):
            for zh in range(2):
                at = q * 32 + zh * 16
                out[pl.ds(to[zh] + 4 + q, 16, stride=16), :] = a[at : at + 16]


def third_kernel(arrived, turns, final_out, marginal_out, final, marginal, sems):
    c0, s0 = angle(turns, 1, 0)
    c2, s2 = angle(turns, 1, 2)
    small = table([(k, k, FLIP, c0, s0) for k in range(6)] + [(6, 6, FLIP, c2, s2)])
    w = doubled(small, FLIP, c2, s2)
    y = mm(w, jnp.concatenate([arrived[pl.ds(k, 256, stride=8), :] for k in range(4)], axis=1))
    own = own_pop()
    quarters = [quarter_turns(own + k) for k in range(3)]
    copies = []
    for t in range(4):
        odd, sign = quarters[bin(t).count("1")]
        odd = odd == 1
        f = []
        for c in range(2):
            part = [y[t * 64 : t * 64 + 64, (c * 2 + lb) * 128 : (c * 2 + lb) * 128 + 128] for lb in range(2)]
            f.append(jnp.concatenate(part, axis=0).T)
        re, im = jnp.where(odd, f[1], f[0]) * sign, jnp.where(odd, -f[0], f[1]) * sign
        for q in range(4):
            final[0, t, pl.ds(q, 32, stride=4), :] = re[q * 32 : q * 32 + 32]
            final[1, t, pl.ds(q, 32, stride=4), :] = im[q * 32 : q * 32 + 32]
        copies.append(pltpu.make_async_copy(final.at[:, t], final_out.at[:, t], sems.at[t]))
        copies[t].start()
    y = mm(w, jnp.concatenate([arrived[pl.ds(4 + k, 256, stride=8), :] for k in range(4)], axis=1))
    pick = jnp.where(bit(iota((8, 128), 1), 5) == iota((8, 128), 0), 1.0 / 32.0, 0.0).astype(jnp.bfloat16)
    upper = iota((1, 128), 1) >= 64
    for q in range(4):
        chance = y[:, q * 128 : q * 128 + 128]
        high, low = halves(chance * chance)
        total = lax.dot_general(
            jnp.concatenate([pick, pick], axis=1),
            jnp.concatenate([high, low], axis=1),
            (((1,), (1,)), ((), ())),
            preferred_element_type=jnp.float32,
        )
        for t in range(4):
            part = total[:, t // 2 * 128 : t // 2 * 128 + 128]
            moved = pltpu.roll(part, 64, 1)
            first, second = (moved, part) if t % 2 else (part, moved)
            marginal[t, q : q + 1, :] = jnp.where(upper, second[1:2], first[0:1])
    copies.append(pltpu.make_async_copy(marginal, marginal_out, sems.at[4]))
    copies[4].start()
    for copy in copies:
        copy.wait()


HERE, AWAY = pl.BlockSpec(memory_space=pltpu.VMEM), pl.BlockSpec(memory_space=pl.ANY)


def inner(*shape):
    return pltpu.VMEM(shape, jnp.float32)


def kept(value):
    return pltpu.with_memory_space_constraint(value, pltpu.VMEM)


def exchange(values, *chunk):
    moved = lax.all_to_all(values.reshape(256, *chunk), GROUP, 0, 0, tiled=True)
    return kept(moved.reshape(values.shape))


def on_device(amplitudes, energies, phase_angles, mix_angles):
    sent, turns = pl.pallas_call(
        first_kernel,
        out_shape=[inner(1536, 128), inner(16, 128)],
        in_specs=[AWAY] * 4,
        out_specs=[HERE, HERE],
        scratch_shapes=[
            inner(2, 4, 128, 128),
            inner(4, 128, 128),
            inner(2, 128),
            pltpu.SMEM((2, 4), jnp.float32),
            pltpu.SemaphoreType.DMA((5,)),
        ],
    )(amplitudes, energies, phase_angles, mix_angles)
    turns = kept(turns)
    arrived = exchange(sent, 3, 2, 128)
    sent = pl.pallas_call(
        second_kernel, out_shape=inner(2048, 128), in_specs=[HERE, HERE], out_specs=HERE
    )(arrived, turns)
    arrived = exchange(sent, 8, 128)
    return pl.pallas_call(
        third_kernel,
        out_shape=[
            jax.ShapeDtypeStruct((2, 4, 128, 128), jnp.float32),
            jax.ShapeDtypeStruct((4, 4, 128), jnp.float32),
        ],
        in_specs=[HERE, HERE],
        out_specs=[AWAY, AWAY],
        scratch_shapes=[inner(2, 4, 128, 128), inner(4, 4, 128), pltpu.SemaphoreType.DMA((5,))],
    )(arrived, turns)


def solution(mesh):
    parted = Mesh(mesh.devices.reshape(2, 4, 4, 4, 2), AXES)
    return jax.shard_map(
        on_device,
        mesh=parted,
        in_specs=(P(None, AXES, None, None), P(AXES, None, None), P(), P()),
        out_specs=(P(None, AXES, None, None), P(AXES[3:], AXES[:3], None)),
        check_vma=False,
    )
```
